32 devices in a mesh: gx: 4 (over z), gy: 4 (over x, core), col: 2 (over y).
Axes of the slice: x: 2, y: 2, z: 4, core: 2. Of those that a mesh axis runs over, the one named last changes fastest.
Arguments:
- fields: bfloat16 [2, 128, 128, 32, 128], P('col', 'gx', 'gy'), may hold values from -6 to 6
- spectral: bfloat16 [1, 16, 16, 2, 32, 32, 16], P(None, 'gx', 'gy', None, None, 'col'), may hold values from -0.75 to 0.75
- skip_weight: bfloat16 [1, 32, 32], replicated, may hold values from -1 to 1
- skip_bias: float32 [1, 32], replicated, may hold values from -3 to 3
- norm_gain: float32 [1, 32], replicated, may hold values from 0.5 to 1.5
- norm_shift: float32 [1, 32], replicated, may hold values from -3 to 3
Outputs:
- activations: bfloat16 [2, 128, 128, 32, 128], P('col', 'gx', 'gy')
The draws below stay inside these ranges and needn't reach their ends.
All inputs are finite; a program needn't handle non-finite values.
Results may differ from the reference program's by a relative error of at most 0.012.
Values may be sent and summed in bfloat16 or wider, within the bound.
A program may use at most 128 MiB of HBM per device.

```python
import math
import jax
import jax.numpy as jnp
from jax import lax

X = 128
Y = 128
Z = 128
C = 32
MX = 16
MY = 16
MZ = 16
LAYERS = 1
SAMPLES = 2


def block_levels(own_key, shape, split, low, largest):
    def one(dim, shards_of):
        draws = jax.random.uniform(jax.random.fold_in(jax.random.fold_in(own_key, 6), dim), (shards_of,), jnp.float32, low / len(split), largest / len(split))
        return jnp.repeat(jnp.exp(draws), shape[dim] // shards_of).reshape((-1,) + (1,) * (len(shape) - dim - 1))

    level = one(*split[0])
    for cut in split[1:]:
        level = level * one(*cut)
    return level


def scatter_about(stream_key, dims, scale, bound, split=(), kind=jnp.bfloat16):
    gain = block_levels(stream_key, dims, split, -0.22, 0.18) if split else 1.0
    array = jax.random.normal(stream_key, dims, jnp.float32) * scale * gain
    return jnp.minimum(jnp.maximum(array, -bound), bound).astype(kind)


def setup_inputs(seed: int = 0) -> dict:
    keys = jax.random.split(jax.random.key(seed), 7)
    fields = scatter_about(keys[0], (SAMPLES, X, Y, C, Z), 1.0, 6.0, ((0, 2), (1, 4), (2, 4)))
    spectral = scatter_about(keys[1], (LAYERS, MX, MY, 2, C, C, MZ), (2 * C) ** -0.5, 0.75, ((1, 4), (2, 4), (5, 2)))
    skip_weight = scatter_about(keys[2], (LAYERS, C, C), C ** -0.5, 1.0)
    skip_bias = scatter_about(keys[3], (LAYERS, C), 0.5, 3.0, (), jnp.float32)
    norm_gain = jnp.clip(jax.random.uniform(keys[4], (LAYERS, C), jnp.float32, 0.5, 1.5), 0.5, 1.5)
    norm_shift = scatter_about(keys[5], (LAYERS, C), 0.5, 3.0, (), jnp.float32)
    return dict(fields=fields, spectral=spectral, skip_weight=skip_weight, skip_bias=skip_bias, norm_gain=norm_gain, norm_shift=norm_shift)


norm_eps = 1e-05

def signed_freqs(count):
    index = jnp.arange(count, dtype=jnp.int32)
    return jnp.where(index < count // 2, index, index - count)

def angles(positions, frequency, length):
    turn_count = positions[:, None] * frequency[None, :] % length
    return turn_count.astype(jnp.float32) * (2.0 * math.pi / length)

def forward_table(positions, frequency, length, factor):
    phase_angle = angles(positions, frequency, length)
    cosine = jnp.cos(phase_angle) * factor
    sine_part = jnp.sin(phase_angle) * factor
    from_real = jnp.stack([cosine, -sine_part], axis=-1)
    from_imag = jnp.stack([sine_part, cosine], axis=-1)
    return jnp.stack([from_real, from_imag], axis=1)

def inverse_table(frequency, positions, length):
    phase_angle = angles(positions, frequency, length).T
    cosine = jnp.cos(phase_angle)
    sine_part = jnp.sin(phase_angle)
    from_real = jnp.stack([cosine, sine_part], axis=-1)
    from_imag = jnp.stack([-sine_part, cosine], axis=-1)
    return jnp.stack([from_real, from_imag], axis=1)

def depth_tables(length, count):
    frequency = jnp.arange(count, dtype=jnp.int32)
    phase_angle = angles(jnp.arange(length, dtype=jnp.int32), frequency, length)
    forward = jnp.concatenate([jnp.cos(phase_angle), -jnp.sin(phase_angle)], axis=1)
    backward = jnp.concatenate([jnp.cos(phase_angle).T, -jnp.sin(phase_angle).T], axis=0)
    return (forward.astype(jnp.bfloat16), backward.astype(jnp.bfloat16))

def mix_modes(spectrum, weight):

    def contract(left, right):
        return jnp.einsum('abcz,abcdz->abdz', left, right, preferred_element_type=jnp.float32, precision=lax.Precision.HIGHEST)
    real_in = spectrum[:, :, :, 0]
    imag_in = spectrum[:, :, :, 1]
    real_weight = weight[:, :, 0]
    imag_weight = weight[:, :, 1]
    real_out = contract(real_in, real_weight) - contract(imag_in, imag_weight)
    imag_out = contract(real_in, imag_weight) + contract(imag_in, real_weight)
    return jnp.stack([real_out, imag_out], axis=3)

def finish(spectral_part, skip_part, offset, scaling, shift_term):
    pre_norm = spectral_part + skip_part + offset[:, None]
    centre = lax.optimization_barrier(jnp.mean(pre_norm, axis=2, keepdims=True))
    spread = lax.optimization_barrier(jnp.mean(jnp.square(pre_norm - centre), axis=2, keepdims=True))
    normed = (pre_norm - centre) * lax.rsqrt(spread + norm_eps) * scaling[:, None] + shift_term[:, None]
    return jax.nn.gelu(normed, approximate=False).astype(jnp.bfloat16)

def sample_layers(sample, spectral, skip_weight, skip_bias, norm_gain, norm_shift):
    highest = lax.Precision.HIGHEST
    depth_forward, depth_backward = depth_tables(Z, MZ)
    first_cells = jnp.arange(X, dtype=jnp.int32)
    second_cells = jnp.arange(Y, dtype=jnp.int32)
    second_forward = forward_table(second_cells, signed_freqs(MY), Y, 1.0).astype(jnp.bfloat16)
    first_forward = forward_table(first_cells, signed_freqs(MX), X, 1.0 / math.sqrt(X * Y * Z))
    first_inverse = inverse_table(signed_freqs(MX), first_cells, X).astype(jnp.bfloat16)
    second_inverse = inverse_table(signed_freqs(MY), second_cells, Y)
    inverse_scale = 1.0 / math.sqrt(MX * MY * MZ)
    hidden = sample
    for layer_index in range(LAYERS):
        amplitude = jnp.dot(hidden.reshape(-1, Z).astype(jnp.float32), depth_forward.astype(jnp.float32), precision=highest)
        amplitude = amplitude.astype(jnp.bfloat16).reshape(X, Y, C, 2, MZ)
        along_second = jnp.einsum('xycrz,yrks->xkcsz', amplitude.astype(jnp.float32), second_forward.astype(jnp.float32), precision=highest)
        spectrum_sum = jnp.einsum('xkcsz,xsjt->jkctz', along_second, first_forward, precision=highest)
        spectrum = spectrum_sum.astype(jnp.bfloat16)
        mixed_modes = mix_modes(spectrum.astype(jnp.float32), spectral[layer_index].astype(jnp.float32)).astype(jnp.bfloat16)
        rows_first = jnp.einsum('jkcsz,jsxt->xkctz', mixed_modes.astype(jnp.float32), first_inverse.astype(jnp.float32), precision=highest)
        rows_both = jnp.einsum('xkcsz,ksyt->xyctz', rows_first, second_inverse, precision=highest).astype(jnp.bfloat16)
        spectral_part = jnp.dot(rows_both.reshape(-1, 2 * MZ).astype(jnp.float32), depth_backward.astype(jnp.float32), precision=highest)
        spectral_part = spectral_part.reshape(X, Y, C, Z) * inverse_scale
        skip_part = jnp.einsum('oc,xycz->xyoz', skip_weight[layer_index].astype(jnp.float32), hidden.astype(jnp.float32), precision=highest)
        hidden = finish(spectral_part, skip_part, skip_bias[layer_index], norm_gain[layer_index], norm_shift[layer_index])
    return hidden

def reference(fields, spectral, skip_weight, skip_bias, norm_gain, norm_shift):

    def per_sample(sample):
        return sample_layers(sample, spectral, skip_weight, skip_bias, norm_gain, norm_shift)
    return lax.map(per_sample, fields)
```

```python
import functools
import math

import jax
import jax.numpy as jnp
import numpy as np
from jax import lax
from jax.experimental import pallas as pl
from jax.experimental.pallas import tpu as pltpu
from jax.sharding import PartitionSpec as P

norm_eps = 1e-05
BF = jnp.bfloat16
F32 = jnp.float32
MESH = pl.DeviceIdType.MESH


def signed(count):
    index = np.arange(count)
    return np.where(index < count // 2, index, index - count)


def cos_sin(positions, frequency, length):
    turns = (positions[:, None] * frequency[None, :]) % length
    phase = turns * (2.0 * math.pi / length)
    return np.cos(phase), np.sin(phase)


def log2(n):
    assert n & (n - 1) == 0
    return n.bit_length() - 1


def div(i, n):
    return lax.shift_right_logical(i, jnp.int32(log2(n)))


def mod(i, n):
    return lax.bitwise_and(i, jnp.int32(n - 1))


def iota(shape, dim):
    return lax.broadcasted_iota(jnp.int32, shape, dim)


def dot(a, b):
    return jnp.dot(a, b, preferred_element_type=F32)


def spread_table(table, width, pick):
    r, c = table.shape
    right = (iota((c, width), 0) == pick(iota((c, width), 1))).astype(F32).astype(BF)
    return dot(table, right)


def band(store, table_ref, rows, height, keep):
    for m in range(rows):
        store(m * height, jnp.where(keep, table_ref[m:m + 1, :], 0.0).astype(BF))


def front_kernel(
    sizes,
    fields_hbm, spectral_hbm, depth_ref, tyf_ref, txf_ref, txi_ref, tyi_ref, skip_ref, bias_ref,
    rows_ref, pre_ref,
    fields_ref, ky_ref, kx_ref, amp_ref, turn_ref, total_ref,
    swap_ref, take_ref, send_ref, recv_ref, mix_ref, modes_ref, gx_ref, hy_ref, w_ref, wa_ref,
    wbd_ref, ty_ref, tx_ref, ti_ref, th_ref,
    fsem, wsem, swap_s, swap_r, send1, recv1, send2, recv2, send3, recv3, send4, recv4,
):
    n_gx, n_gy, n_col, xl, yl, C, MY, MZ, kxl, kyl, dl, G, steps, halves, tile = sizes
    n_hi = n_gy // 2
    peers = n_gx * n_hi
    MX = n_gx * kxl
    L = 2 * kxl * MZ
    CH = C // halves
    per = n_col // halves
    Z = fields_ref.shape[-1]
    block = kyl * CH
    top = MY * CH
    gx, gy, col = lax.axis_index("gx"), lax.axis_index("gy"), lax.axis_index("col")
    lo, hi = lax.rem(gy, 2), lax.div(gy, 2)
    mate = gy + 1 - 2 * lo
    unrolled = peers <= 16

    def peer(i):
        return lax.rem(gx + i // n_hi, n_gx), lax.rem(hi + i % n_hi, n_hi)

    def source(i):
        return lax.rem(gx + n_gx - i // n_hi, n_gx), lax.rem(hi + n_hi - i % n_hi, n_hi)

    def side(i):
        return lax.rem(col + i, n_col)

    def loop(low, high, body):
        if unrolled:
            for i in range(low, high):
                body(i)
            return

        def go(i, carry):
            body(i)
            return carry
        lax.fori_loop(low, high, go, 0)

    def field_copy(h, s):
        at = (pl.ds(s * G, G), slice(None), pl.ds(h * CH, CH), slice(None))
        return pltpu.make_async_copy(fields_hbm.at[at], fields_ref.at[at], fsem.at[h, s])

    weights_copy = pltpu.make_async_copy(spectral_hbm, w_ref, wsem)
    units = [(h, s) for h in range(halves) for s in range(steps)]
    field_copy(*units[0]).start()
    weights_copy.start()
    for unit in units[1:]:
        field_copy(*unit).start()

    barrier = pltpu.get_barrier_semaphore()

    def greet(i):
        px, ph = peer(i)
        pl.semaphore_signal(
            barrier, inc=1, device_id={"gx": px, "gy": 2 * ph + lo}, device_id_type=MESH
        )

    def greet_side(i):
        pl.semaphore_signal(barrier, inc=1, device_id={"col": side(i)}, device_id_type=MESH)

    loop(1, peers, greet)
    loop(1, n_col, greet_side)
    pl.semaphore_signal(barrier, inc=1, device_id={"gy": mate}, device_id_type=MESH)

    ty_ref[...] = spread_table(tyf_ref[gy], yl * CH, lambda j: div(j, CH))
    tx_ref[...] = spread_table(txf_ref[gx], 2 * MX * MZ, lambda j: div(j, MZ))

    def put_ky(first, value):
        ky_ref[pl.ds(first, CH), :] = value

    band(put_ky, ty_ref, 2 * MY, CH, iota((CH, yl * CH), 0) == mod(iota((CH, yl * CH), 1), CH))

    def put_kx(first, value):
        kx_ref[pl.ds(first, MZ), :] = value

    wide = 2 * MX * MZ
    band(put_kx, tx_ref, 4 * steps * G, MZ, iota((MZ, wide), 0) == mod(iota((MZ, wide), 1), MZ))

    def share(i):
        return pltpu.make_async_remote_copy(
            src_ref=wa_ref.at[col], dst_ref=wa_ref.at[col],
            send_sem=send2.at[i], recv_sem=recv2.at[i],
            device_id={"col": side(i)}, device_id_type=MESH,
        )

    def swap(h):
        return pltpu.make_async_remote_copy(
            src_ref=swap_ref.at[h], dst_ref=take_ref.at[h],
            send_sem=swap_s.at[h], recv_sem=swap_r.at[h],
            device_id={"gy": mate}, device_id_type=MESH,
        )

    def scatter(h, i):
        px, ph = peer(i)
        return pltpu.make_async_remote_copy(
            src_ref=send_ref.at[h, px, ph], dst_ref=recv_ref.at[h, i],
            send_sem=send1.at[h, i], recv_sem=recv1.at[h, i],
            device_id={"gx": px, "gy": 2 * ph + lo}, device_id_type=MESH,
        )

    def gather(i):
        px, ph = peer(i)
        return pltpu.make_async_remote_copy(
            src_ref=mix_ref, dst_ref=modes_ref.at[gx, gy],
            send_sem=send3.at[i], recv_sem=recv3.at[i],
            device_id={"gx": px, "gy": 2 * ph + lo}, device_id_type=MESH,
        )

    def relay(i):
        if isinstance(i, int) and i == 0:
            src, at = mix_ref, modes_ref.at[gx, gy]
        else:
            sx, sh = source(i)
            src = at = modes_ref.at[sx, 2 * sh + lo]
        return pltpu.make_async_remote_copy(
            src_ref=src, dst_ref=at, send_sem=send4.at[i], recv_sem=recv4.at[i],
            device_id={"gy": mate}, device_id_type=MESH,
        )

    def prepare_weights():
        weights_copy.wait()
        eye = (iota((C, C), 0) == iota((C, C), 1)).astype(F32).astype(BF)
        for k in range(kyl):
            for d in range(dl):
                parts = [w_ref[j, k, r, d] for r in range(2) for j in range(kxl)]
                wa_ref[col, k, d] = lax.dot_general(
                    eye, jnp.concatenate(parts, axis=0), (((1,), (1,)), ((), ())),
                    preferred_element_type=F32,
                ).astype(BF)
        pl.semaphore_wait(barrier, peers + n_col - 1)
        for i in range(1, n_col):
            share(i).start()

    def z_stage(u):
        h, s = units[u]
        field_copy(h, s).wait()
        lhs = jnp.concatenate(
            [fields_ref[s * G + g, :, h * CH:(h + 1) * CH, :].reshape(yl * CH, Z) for g in range(G)],
            axis=-1,
        )
        amp_ref[u % 2] = dot(lhs, depth_ref[...]).astype(BF)

    def y_stage(u):
        h, s = units[u]
        lanes = 2 * G * MZ
        turn_ref[h % 2, :, s * lanes:(s + 1) * lanes] = dot(ky_ref[...], amp_ref[u % 2]).astype(BF)

    piece = min(2, steps)

    def x_stage(u):
        h, s = units[u]
        if s % piece != piece - 1:
            return
        lanes = piece * 2 * G * MZ
        cut = slice((s + 1) * 2 * G * MZ - lanes, (s + 1) * 2 * G * MZ)
        count = steps * 2 * G * MZ
        term = dot(turn_ref[h % 2, :top, cut], kx_ref[cut.start:cut.stop, :])
        term = term + dot(turn_ref[h % 2, top:, cut], kx_ref[count + cut.start:count + cut.stop, :])
        if s == piece - 1:
            total_ref[h % 2] = term
        else:
            total_ref[h % 2] += term
        if s == steps - 1:
            for i in range(n_hi):
                at = pl.multiple_of((2 * i + 1 - lo) * block, block)
                swap_ref[h, i] = total_ref[h % 2, pl.ds(at, block), :].astype(BF)
            swap(h).start()

    def send_half(h):
        swap(h).wait_recv()
        for i in range(n_hi):
            at = pl.multiple_of((2 * i + lo) * block, block)
            value = total_ref[h % 2, pl.ds(at, block), :] + take_ref[h, i].astype(F32)
            value = value.astype(BF)
            for b in range(n_gx):
                send_ref[h, b, i] = value[:, b * L:(b + 1) * L]
        loop(1, peers, lambda i: scatter(h, i).start())

    ready = min(2, len(units))
    for u in range(len(units) + 2):
        if u == ready:
            prepare_weights()
        if u < len(units):
            z_stage(u)
        if 0 <= u - 1 < len(units):
            y_stage(u - 1)
        if 0 <= u - 2:
            x_stage(u - 2)
        if halves > 1 and u == steps + 3:
            send_half(0)

    weight = skip_ref[...].astype(F32)
    weight = (weight - jnp.mean(weight, axis=0, keepdims=True)).astype(BF)
    tall = spread_table(weight, tile, lambda j: mod(j, C))
    for g in range(tile // C):
        keep = div(iota((C, tile), 1), C) == g
        wbd_ref[g * C:(g + 1) * C, :] = jnp.where(keep, tall, 0.0).astype(BF)
    diagonal = iota((C, C), 0) == iota((C, C), 1)
    bias = jnp.sum(jnp.where(diagonal, bias_ref[...], 0.0), 1, keepdims=True)
    bias = (bias - jnp.mean(bias, axis=0, keepdims=True))[None]

    def skip_cells(low, high):
        def go(i, carry):
            x = 2 * i
            for y in range(0, yl, tile // C):
                hidden = jnp.concatenate(
                    [fields_ref[x + k, y:y + tile // C].reshape(tile, Z) for k in range(2)], axis=-1
                )
                part = dot(wbd_ref[...], hidden).reshape(tile // C, C, 2 * Z) + bias
                for k in range(2):
                    pre_ref[x + k, y:y + tile // C] = part[:, :, k * Z:(k + 1) * Z]
            return carry
        lax.fori_loop(low, high, go, 0)

    pairs = xl // 2
    skip_cells(0, pairs // 8)
    send_half(halves - 1)

    ti_ref[...] = spread_table(txi_ref[gx], 2 * xl * MZ, lambda j: div(j, MZ))
    th_ref[...] = spread_table(
        tyi_ref[gy], 2 * MY * CH,
        lambda j: div(j, per * kyl * dl) * kyl + mod(div(j, dl), kyl),
    )

    def put_gx(first, value):
        gx_ref[pl.ds(first, MZ), :] = value

    wide = 2 * xl * MZ
    band(put_gx, ti_ref, 4 * MX, MZ, iota((MZ, wide), 0) == mod(iota((MZ, wide), 1), MZ))

    def put_hy(first, value):
        hy_ref[pl.ds(first, CH), :] = value

    j = iota((CH, 2 * MY * CH), 1)
    band(
        put_hy, th_ref, yl, CH,
        iota((CH, 2 * MY * CH), 0) == mod(div(j, kyl * dl), per) * dl + mod(j, dl),
    )
    skip_cells(pairs // 8, pairs // 2)

    sums = {}
    for h in range(halves):
        total = send_ref[h, gx, hi].astype(F32)
        for i in range(1, peers):
            scatter(h, i).wait_recv()
            total = total + recv_ref[h, i].astype(F32)
        spec = total.astype(BF).astype(F32)
        if h == 0:
            for i in range(1, n_col):
                share(i).wait_recv()
        re, im = spec[:, :L // 2], spec[:, L // 2:]
        re = jnp.concatenate([re, re], axis=-1)
        im = jnp.concatenate([im, im], axis=-1)
        for q in range(n_col):
            for k in range(kyl):
                rows, chans = slice(k * CH, (k + 1) * CH), slice(h * CH, (h + 1) * CH)
                weight = wa_ref[q, k, :, chans].astype(F32)
                new = [jnp.sum(v[rows][None] * weight, axis=1) for v in (re, im)]
                old = sums.get((q, k))
                sums[q, k] = new if old is None else [a + b for a, b in zip(old, new)]
    for k in range(kyl):
        mixed = []
        for q in range(n_col):
            first, second = sums[q, k]
            turned_second = jnp.concatenate(
                [-second[:, L // 2:], second[:, :L // 2]], axis=-1
            )
            mixed.append(first + turned_second)
        centre = sum(jnp.sum(m, axis=0, keepdims=True) for m in mixed) * (1.0 / C)
        for q in range(n_col):
            row = (q * kyl + k) * dl
            mix_ref[row:row + dl] = (mixed[q] - centre).astype(BF)

    loop(1, peers, lambda i: gather(i).start())
    relay(0).start()
    modes_ref[gx, gy] = mix_ref[...]
    skip_cells(pairs // 2, pairs)

    def pass_on(i):
        gather(i).wait_recv()
        relay(i).start()

    loop(1, peers, pass_on)
    for h in range(halves):
        swap(h).wait_send()
        loop(1, peers, lambda i: scatter(h, i).wait_send())
    for i in range(1, n_col):
        share(i).wait_send()
    relay(0).wait_recv()
    loop(1, peers, lambda i: relay(i).wait_recv())

    span = kyl * CH
    lanes = rows_ref.shape[-1]
    for h in range(halves):
        part = jnp.concatenate(
            [
                jnp.concatenate([modes_ref[b, g, h * span:(h + 1) * span] for g in range(n_gy)], axis=0)
                for b in range(n_gx)
            ],
            axis=-1,
        )
        half = 2 * MX * MZ
        part = jnp.concatenate(
            [dot(part, gx_ref[cs * half:(cs + 1) * half, :]).astype(BF) for cs in range(2)], axis=0
        )
        value = dot(hy_ref[...], part).astype(BF).reshape(yl, CH, 2 * xl * MZ)
        for g in range(rows_ref.shape[0]):
            rows_ref[g, :, h * CH:(h + 1) * CH] = value[:, :, g * lanes:(g + 1) * lanes]
    relay(0).wait_send()
    loop(1, peers, lambda i: gather(i).wait_send())
    loop(1, peers, lambda i: relay(i).wait_send())


def back_kernel(sizes, rows_ref, pre_ref, depth_ref, gain_ref, shift_ref, out_hbm, out_ref, sem):
    groups, G, yl, C, Z, cells = sizes

    def column(ref):
        return jnp.sum(jnp.where(iota((C, C), 0) == iota((C, C), 1), ref[...], 0.0), 1, keepdims=True)

    root = 0.5 ** 0.5
    gain = (column(gain_ref) * root)[None]
    shift = (column(shift_ref) * root)[None]

    def leave(i, slot):
        return pltpu.make_async_copy(
            out_ref.at[slot], out_hbm.at[pl.ds(i * G, G)], sem.at[slot]
        )

    def go(i, carry):
        slot = mod(i, 2)

        @pl.when(i >= 2)
        def _():
            leave(i - 2, slot).wait()

        for y in range(0, yl, cells):
            part = dot(rows_ref[i, y:y + cells].reshape(cells * C, rows_ref.shape[-1]), depth_ref[...])
            for k in range(G):
                pre = part[:, k * Z:(k + 1) * Z].reshape(cells, C, Z) + pre_ref[i * G + k, y:y + cells]
                spread = jnp.mean(pre * pre, axis=1, keepdims=True)
                value = (pre * (lax.rsqrt(spread + norm_eps) * gain) + shift).astype(BF)
                value = (value * root).astype(BF) * (1.0 + lax.erf(value)).astype(BF)
                out_ref[slot, k, y:y + cells] = value
        leave(i, slot).start()
        return carry

    lax.fori_loop(0, groups, go, 0)
    for i in range(max(0, groups - 2), groups):
        leave(i, i % 2).wait()


def build(mesh):
    n_gx, n_gy, n_col = (mesh.shape[a] for a in ("gx", "gy", "col"))

    def local(fields, spectral, skip_weight, skip_bias, norm_gain, norm_shift):
        hidden = fields[0]
        xl, yl, C, Z = hidden.shape
        weights = spectral[0]
        kxl, kyl, _, _, dl, MZ = weights.shape
        X, Y, MX, MY = xl * n_gx, yl * n_gy, kxl * n_gx, kyl * n_gy
        G = min(8, xl)
        steps = xl // G
        L = 2 * kxl * MZ
        n_hi = n_gy // 2
        peers = n_gx * n_hi
        G2 = min(4, xl)

        cz, sz = cos_sin(np.arange(Z), np.arange(MZ), Z)
        forward = np.concatenate([cz, -sz], axis=1)
        depth_forward = np.kron(np.eye(G), forward)
        backward = np.concatenate([cz.T, -sz.T], axis=0) / math.sqrt(MX * MY * MZ)
        depth_backward = np.kron(np.eye(G2), backward)
        cy, sy = cos_sin(np.arange(Y), signed(MY), Y)
        tyf = np.stack([cy, sy]).reshape(2, n_gy, yl, MY).transpose(1, 0, 3, 2)
        tyf = tyf.reshape(n_gy, 2 * MY, yl)
        tyi = np.stack([cy, sy]).reshape(2, n_gy, yl, MY).transpose(1, 2, 0, 3)
        tyi = tyi.reshape(n_gy, yl, 2 * MY)
        cx, sx = cos_sin(np.arange(X), signed(MX), X)
        f = np.stack([
            np.stack([np.stack([cx, -sx], 1), np.stack([sx, cx], 1)], 1),
            np.stack([np.stack([-sx, -cx], 1), np.stack([cx, -sx], 1)], 1),
        ]) / math.sqrt(X * Y * Z)
        f = f.reshape(2, n_gx, xl, 2, 2, n_gx, kxl).transpose(1, 0, 2, 3, 5, 4, 6)
        txf = f.reshape(n_gx, 4 * xl, 2 * MX)
        b = np.stack([
            np.stack([np.stack([cx, sx]), np.stack([-sx, cx])]),
            np.stack([np.stack([-sx, cx]), np.stack([-cx, -sx])]),
        ])
        b = b.reshape(2, 2, 2, n_gx, xl, n_gx, kxl).transpose(3, 0, 5, 1, 6, 4, 2)
        txi = b.reshape(n_gx, 4 * MX, 2 * xl)
        const = lambda a: jnp.asarray(a.astype(np.float32)).astype(BF)

        halves = 2 if C % 32 == 0 and n_col % 2 == 0 else 1
        CH = C // halves
        turned = jnp.transpose(weights, (0, 1, 2, 4, 5, 3))
        tile = min(256, yl * C)

        sizes = (n_gx, n_gy, n_col, xl, yl, C, MY, MZ, kxl, kyl, dl, G, steps, halves, tile)
        tables = [const(t) for t in (depth_forward, tyf, txf, txi, tyi)]
        inside = pl.BlockSpec(memory_space=pltpu.VMEM)
        outside = pl.BlockSpec(memory_space=pltpu.HBM)
        rows_both, pre = pl.pallas_call(
            functools.partial(front_kernel, sizes),
            out_shape=(
                pltpu.VMEM((xl // G2, yl, C, G2 * 2 * MZ), BF),
                pltpu.VMEM((xl, yl, C, Z), F32),
            ),
            in_specs=[outside, outside] + [inside] * (len(tables) + 2),
            out_specs=(inside, inside),
            scratch_shapes=[
                pltpu.VMEM((xl, yl, C, Z), BF),
                pltpu.VMEM((2 * MY * CH, yl * CH), BF),
                pltpu.VMEM((4 * xl * MZ, 2 * MX * MZ), BF),
                pltpu.VMEM((2, yl * CH, G * 2 * MZ), BF),
                pltpu.VMEM((2, 2 * MY * CH, xl * 2 * MZ), BF),
                pltpu.VMEM((2, MY * CH, 2 * MX * MZ), F32),
                pltpu.VMEM((halves, n_hi, kyl * CH, n_gx * L), BF),
                pltpu.VMEM((halves, n_hi, kyl * CH, n_gx * L), BF),
                pltpu.VMEM((halves, n_gx, n_hi, kyl * CH, L), BF),
                pltpu.VMEM((halves, peers, kyl * CH, L), BF),
                pltpu.VMEM((kyl * C, L), BF),
                pltpu.VMEM((n_gx, n_gy, kyl * C, L), BF),
                pltpu.VMEM((4 * MX * MZ, 2 * xl * MZ), BF),
                pltpu.VMEM((yl * CH, 2 * MY * CH), BF),
                pltpu.VMEM(turned.shape, BF),
                pltpu.VMEM((n_col, kyl, dl, C, L), BF),
                pltpu.VMEM((tile, tile), BF),
                pltpu.VMEM((2 * MY, yl * CH), F32),
                pltpu.VMEM((4 * xl, 2 * MX * MZ), F32),
                pltpu.VMEM((4 * MX, 2 * xl * MZ), F32),
                pltpu.VMEM((yl, 2 * MY * CH), F32),
                pltpu.SemaphoreType.DMA((halves, steps)),
                pltpu.SemaphoreType.DMA,
                pltpu.SemaphoreType.DMA((halves,)),
                pltpu.SemaphoreType.DMA((halves,)),
                pltpu.SemaphoreType.DMA((halves, peers)),
                pltpu.SemaphoreType.DMA((halves, peers)),
                pltpu.SemaphoreType.DMA((n_col,)),
                pltpu.SemaphoreType.DMA((n_col,)),
                pltpu.SemaphoreType.DMA((peers,)),
                pltpu.SemaphoreType.DMA((peers,)),
                pltpu.SemaphoreType.DMA((peers,)),
                pltpu.SemaphoreType.DMA((peers,)),
            ],
            compiler_params=pltpu.CompilerParams(
                collective_id=0, has_side_effects=True, vmem_limit_bytes=40 * 2**20,
            ),
            name="front",
        )(hidden, turned, *tables, skip_weight[0], skip_bias)

        groups = xl // G2
        cells = min(8, yl)
        out = pl.pallas_call(
            functools.partial(back_kernel, (groups, G2, yl, C, Z, cells)),
            out_shape=jax.ShapeDtypeStruct(hidden.shape, BF),
            in_specs=[inside] * 5,
            out_specs=outside,
            scratch_shapes=[
                pltpu.VMEM((2, G2, yl, C, Z), BF),
                pltpu.SemaphoreType.DMA((2,)),
            ],
            compiler_params=pltpu.CompilerParams(vmem_limit_bytes=12 * 2**20),
            name="back",
        )(rows_both, pre, const(depth_backward), norm_gain, norm_shift)
        return out[None]

    return local


def solution(mesh):
    placed = (
        P("col", "gx", "gy", None, None),
        P(None, "gx", "gy", None, None, "col", None),
        P(), P(), P(), P(),
    )
    return jax.shard_map(
        build(mesh), mesh=mesh, in_specs=placed,
        out_specs=P("col", "gx", "gy", None, None), check_vma=False,
    )
```

```python
import functools
import math

import jax
import jax.numpy as jnp
import numpy as np
from jax import lax
from jax.experimental import pallas as pl
from jax.experimental.pallas import tpu as pltpu
from jax.sharding import PartitionSpec as P

norm_eps = 1e-05
BF = jnp.bfloat16
F32 = jnp.float32
MESH = pl.DeviceIdType.MESH


def signed(count):
    index = np.arange(count)
    return np.where(index < count // 2, index, index - count)


def cos_sin(positions, frequency, length):
    turns = (positions[:, None] * frequency[None, :]) % length
    phase = turns * (2.0 * math.pi / length)
    return np.cos(phase), np.sin(phase)


def log2(n):
    assert n & (n - 1) == 0
    return n.bit_length() - 1


def div(i, n):
    return lax.shift_right_logical(i, jnp.int32(log2(n)))


def mod(i, n):
    return lax.bitwise_and(i, jnp.int32(n - 1))


def iota(shape, dim):
    return lax.broadcasted_iota(jnp.int32, shape, dim)


def dot(a, b):
    return jnp.dot(a, b, preferred_element_type=F32)


def spread_table(table, width, pick):
    r, c = table.shape
    right = (iota((c, width), 0) == pick(iota((c, width), 1))).astype(F32).astype(BF)
    return dot(table, right)


def per_dl(dl, n_col, halves):
    return n_col == halves and dl % 8 == 0


def band(store, table_ref, rows, height, keep):
    for m in range(rows):
        store(m * height, jnp.where(keep, table_ref[m:m + 1, :], 0.0).astype(BF))


def front_kernel(
    sizes,
    fields_hbm, spectral_hbm, depth_ref, tyf_ref, txf_ref, txi_ref, tyi_ref, skip_ref, bias_ref, gain_ref,
    rows_ref, pre_ref,
    fields_ref, ky_ref, kx_ref, amp_ref, turn_ref, total_ref,
    swap_ref, take_ref, send_ref, recv_ref, mix_ref, modes_ref, gx_ref, hy_ref, w_ref, wa_ref,
    wbd_ref, ty_ref, tx_ref, ti_ref, th_ref,
    fsem, wsem, swap_s, swap_r, send1, recv1, send2, recv2, send3, recv3, send4, recv4,
):
    n_gx, n_gy, n_col, xl, yl, C, MY, MZ, kxl, kyl, dl, G, steps, halves, tile = sizes
    n_hi = n_gy // 2
    peers = n_gx * n_hi
    MX = n_gx * kxl
    L = 2 * kxl * MZ
    CH = C // halves
    CS = 8 if CH % 8 == 0 else CH
    per = n_col // halves
    Z = fields_ref.shape[-1]
    block = kyl * CH
    top = MY * CH
    gx, gy, col = lax.axis_index("gx"), lax.axis_index("gy"), lax.axis_index("col")
    lo, hi = lax.rem(gy, 2), lax.div(gy, 2)
    mate = gy + 1 - 2 * lo
    unrolled = peers <= 16

    def peer(i):
        return lax.rem(gx + i // n_hi, n_gx), lax.rem(hi + i % n_hi, n_hi)

    def source(i):
        return lax.rem(gx + n_gx - i // n_hi, n_gx), lax.rem(hi + n_hi - i % n_hi, n_hi)

    def side(i):
        return lax.rem(col + i, n_col)

    def loop(low, high, body):
        if unrolled:
            for i in range(low, high):
                body(i)
            return

        def go(i, carry):
            body(i)
            return carry
        lax.fori_loop(low, high, go, 0)

    def field_copy(h, s):
        at = (pl.ds(s * G, G), slice(None), pl.ds(h * CH, CH), slice(None))
        return pltpu.make_async_copy(fields_hbm.at[at], fields_ref.at[at], fsem.at[h, s])

    weights_copy = pltpu.make_async_copy(spectral_hbm, w_ref, wsem)
    units = [(h, s) for h in range(halves) for s in range(steps)]
    field_copy(*units[0]).start()
    weights_copy.start()
    for unit in units[1:3]:
        field_copy(*unit).start()

    barrier = pltpu.get_barrier_semaphore()

    def greet(i):
        px, ph = peer(i)
        pl.semaphore_signal(
            barrier, inc=1, device_id={"gx": px, "gy": 2 * ph + lo}, device_id_type=MESH
        )

    def greet_side(i):
        pl.semaphore_signal(barrier, inc=1, device_id={"col": side(i)}, device_id_type=MESH)

    loop(1, peers, greet)
    loop(1, n_col, greet_side)
    pl.semaphore_signal(barrier, inc=1, device_id={"gy": mate}, device_id_type=MESH)

    ty_ref[...] = spread_table(tyf_ref[gy], yl * CS, lambda j: div(j, CS))
    tx_ref[...] = spread_table(txf_ref[gx], 2 * MX * MZ, lambda j: div(j, MZ))

    def put_ky(first, value):
        ky_ref[pl.ds(first, CS), :] = value

    band(put_ky, ty_ref, 2 * MY, CS, iota((CS, yl * CS), 0) == mod(iota((CS, yl * CS), 1), CS))

    def put_kx(first, value):
        kx_ref[pl.ds(first, MZ), :] = value

    wide = 2 * MX * MZ
    band(put_kx, tx_ref, 4 * steps * G, MZ, iota((MZ, wide), 0) == mod(iota((MZ, wide), 1), MZ))

    def share(i, k):
        return pltpu.make_async_remote_copy(
            src_ref=wa_ref.at[col, k], dst_ref=wa_ref.at[col, k],
            send_sem=send2.at[i, k], recv_sem=recv2.at[i, k],
            device_id={"col": side(i)}, device_id_type=MESH,
        )

    def swap(h):
        return pltpu.make_async_remote_copy(
            src_ref=swap_ref.at[h], dst_ref=take_ref.at[h],
            send_sem=swap_s.at[h], recv_sem=swap_r.at[h],
            device_id={"gy": mate}, device_id_type=MESH,
        )

    def scatter(h, i):
        px, ph = peer(i)
        return pltpu.make_async_remote_copy(
            src_ref=send_ref.at[h, px, ph], dst_ref=recv_ref.at[h, i],
            send_sem=send1.at[h, i], recv_sem=recv1.at[h, i],
            device_id={"gx": px, "gy": 2 * ph + lo}, device_id_type=MESH,
        )

    span = kyl * C // halves

    def gather(h, i):
        px, ph = peer(i)
        cut = pl.ds(h * span, span)
        return pltpu.make_async_remote_copy(
            src_ref=mix_ref.at[cut], dst_ref=modes_ref.at[gx, gy, cut],
            send_sem=send3.at[h, i], recv_sem=recv3.at[h, i],
            device_id={"gx": px, "gy": 2 * ph + lo}, device_id_type=MESH,
        )

    def relay(h, i):
        cut = pl.ds(h * span, span)
        if isinstance(i, int) and i == 0:
            src, at = mix_ref.at[cut], modes_ref.at[gx, gy, cut]
        else:
            sx, sh = source(i)
            src = at = modes_ref.at[sx, 2 * sh + lo, cut]
        return pltpu.make_async_remote_copy(
            src_ref=src, dst_ref=at, send_sem=send4.at[h, i], recv_sem=recv4.at[h, i],
            device_id={"gy": mate}, device_id_type=MESH,
        )

    def prepare_weights():
        weights_copy.wait()
        eye = (iota((C, C), 0) == iota((C, C), 1)).astype(F32).astype(BF)
        for k in range(kyl):
            for d in range(dl):
                parts = [w_ref[j, k, r, d] for r in range(2) for j in range(kxl)]
                wa_ref[col, k, d] = lax.dot_general(
                    eye, jnp.concatenate(parts, axis=0), (((1,), (1,)), ((), ())),
                    preferred_element_type=F32,
                ).astype(BF)

    def z_stage(u):
        h, s = units[u]
        field_copy(h, s).wait()
        if u + 3 < len(units):
            field_copy(*units[u + 3]).start()
        lhs = jnp.concatenate(
            [fields_ref[s * G + g, :, h * CH:(h + 1) * CH, :].reshape(yl * CH, Z) for g in range(G)],
            axis=-1,
        )
        value = dot(lhs, depth_ref[...]).reshape(yl, CH // CS, CS, 2 * G * MZ)
        for e in range(CH // CS):
            amp_ref[u % 2, e] = value[:, e].reshape(yl * CS, 2 * G * MZ).astype(BF)

    def y_stage(u):
        h, s = units[u]
        lanes = 2 * G * MZ
        value = jnp.concatenate(
            [
                dot(ky_ref[...], amp_ref[u % 2, e]).reshape(2 * MY, CS, lanes)
                for e in range(CH // CS)
            ],
            axis=1,
        )
        turn_ref[h % 2, :, s * lanes:(s + 1) * lanes] = value.reshape(2 * MY * CH, lanes).astype(BF)

    piece = 1

    def x_stage(u):
        h, s = units[u]
        if s % piece != piece - 1:
            return
        lanes = piece * 2 * G * MZ
        cut = slice((s + 1) * 2 * G * MZ - lanes, (s + 1) * 2 * G * MZ)
        count = steps * 2 * G * MZ
        term = dot(turn_ref[h % 2, :top, cut], kx_ref[cut.start:cut.stop, :])
        term = term + dot(turn_ref[h % 2, top:, cut], kx_ref[count + cut.start:count + cut.stop, :])
        if s == piece - 1:
            total_ref[h % 2] = term
        else:
            total_ref[h % 2] += term
        if s == steps - 1:
            for i in range(n_hi):
                at = pl.multiple_of((2 * i + 1 - lo) * block, block)
                swap_ref[h, i] = total_ref[h % 2, pl.ds(at, block), :].astype(BF)
            swap(h).start()

    def send_half(h):
        swap(h).wait_recv()
        for i in range(n_hi):
            at = pl.multiple_of((2 * i + lo) * block, block)
            value = total_ref[h % 2, pl.ds(at, block), :] + take_ref[h, i].astype(F32)
            value = value.astype(BF)
            for b in range(n_gx):
                send_ref[h, b, i] = value[:, b * L:(b + 1) * L]
        loop(1, peers, lambda i: scatter(h, i).start())

    for u in range(len(units) + 1):
        if u < len(units):
            z_stage(u)
        if u == 0:
            prepare_weights()
            pl.semaphore_wait(barrier, peers + n_col - 1)
            for k in range(kyl):
                for i in range(1, n_col):
                    share(i, k).start()
        if 0 <= u - 1:
            y_stage(u - 1)
            x_stage(u - 1)
        if halves > 1 and u == steps + 1:
            send_half(0)

    weight = skip_ref[...].astype(F32)
    weight = (weight - jnp.mean(weight, axis=0, keepdims=True)).astype(BF)
    tall = spread_table(weight, tile, lambda j: mod(j, C))
    for g in range(tile // C):
        keep = div(iota((C, tile), 1), C) == g
        wbd_ref[g * C:(g + 1) * C, :] = jnp.where(keep, tall, 0.0).astype(BF)
    diagonal = iota((C, C), 0) == iota((C, C), 1)
    bias = jnp.sum(jnp.where(diagonal, bias_ref[...], 0.0), 1, keepdims=True)
    gain = jnp.sum(jnp.where(diagonal, gain_ref[...], 0.0), 1, keepdims=True) * (0.5 ** 0.5)
    bias = ((bias - jnp.mean(bias, axis=0, keepdims=True)) * gain)[None]

    def skip_cells(low, high):
        def go(i, carry):
            x = 2 * i
            for y in range(0, yl, tile // C):
                hidden = jnp.concatenate(
                    [fields_ref[x + k, y:y + tile // C].reshape(tile, Z) for k in range(2)], axis=-1
                )
                part = dot(wbd_ref[...], hidden).reshape(tile // C, C, 2 * Z) * gain[None] + bias
                for k in range(2):
                    pre_ref[x + k, y:y + tile // C] = part[:, :, k * Z:(k + 1) * Z]
            return carry
        lax.fori_loop(low, high, go, 0)

    pairs = xl // 2
    early, mid = pairs // 8, pairs // 2
    skip_cells(0, early)
    send_half(halves - 1)

    ti_ref[...] = spread_table(txi_ref[gx], 2 * xl * MZ, lambda j: div(j, MZ))
    DS = 8 if per_dl(dl, n_col, halves) else CH
    th_ref[...] = spread_table(
        tyi_ref[gy], 2 * MY * DS,
        (lambda j: div(j, DS)) if DS < CH else
        (lambda j: div(j, per * kyl * dl) * kyl + mod(div(j, dl), kyl)),
    )

    def put_gx(first, value):
        gx_ref[pl.ds(first, MZ), :] = value

    wide = 2 * xl * MZ
    band(put_gx, ti_ref, 4 * MX, MZ, iota((MZ, wide), 0) == mod(iota((MZ, wide), 1), MZ))

    def put_hy(first, value):
        hy_ref[pl.ds(first, DS), :] = value

    j = iota((DS, 2 * MY * DS), 1)
    chan = mod(j, DS) if DS < CH else mod(div(j, kyl * dl), per) * dl + mod(j, dl)
    band(put_hy, th_ref, yl, DS, iota((DS, 2 * MY * DS), 0) == chan)
    skip_cells(early, early + mid)

    sums = {}
    for h in range(halves):
        total = send_ref[h, gx, hi].astype(F32)
        for i in range(1, peers):
            scatter(h, i).wait_recv()
            total = total + recv_ref[h, i].astype(F32)
        spec = total.astype(BF).astype(F32)
        if h == 0:
            for i in range(1, n_col):
                for k in range(kyl):
                    share(i, k).wait_recv()
        re, im = spec[:, :L // 2], spec[:, L // 2:]
        re = jnp.concatenate([re, re], axis=-1)
        im = jnp.concatenate([im, im], axis=-1)
        for q in range(n_col):
            for k in range(kyl):
                rows, chans = slice(k * CH, (k + 1) * CH), slice(h * CH, (h + 1) * CH)
                weight = wa_ref[q, k, :, chans].astype(F32)
                new = [jnp.sum(v[rows][None] * weight, axis=1) for v in (re, im)]
                old = sums.get((q, k))
                sums[q, k] = new if old is None else [a + b for a, b in zip(old, new)]
    for k in range(kyl):
        mixed = []
        for q in range(n_col):
            first, second = sums[q, k]
            turned_second = jnp.concatenate(
                [-second[:, L // 2:], second[:, :L // 2]], axis=-1
            )
            mixed.append(first + turned_second)
        centre = sum(jnp.sum(m, axis=0, keepdims=True) for m in mixed) * (1.0 / C)
        for q in range(n_col):
            row = (q * kyl + k) * dl
            mix_ref[row:row + dl] = ((mixed[q] - centre) * gain[q * dl:(q + 1) * dl]).astype(BF)

    for h in range(halves):
        loop(1, peers, lambda i: gather(h, i).start())
        relay(h, 0).start()
    modes_ref[gx, gy] = mix_ref[...]
    skip_cells(early + mid, pairs)
    for h in range(halves):
        swap(h).wait_send()
        loop(1, peers, lambda i: scatter(h, i).wait_send())
    for i in range(1, n_col):
        for k in range(kyl):
            share(i, k).wait_send()

    lanes = rows_ref.shape[-1]
    for h in range(halves):
        def pass_on(i):
            gather(h, i).wait_recv()
            relay(h, i).start()

        loop(1, peers, pass_on)

    for h in range(halves):
        relay(h, 0).wait_recv()
        loop(1, peers, lambda i: relay(h, i).wait_recv())
        part = jnp.concatenate(
            [
                jnp.concatenate([modes_ref[b, g, h * span:(h + 1) * span] for g in range(n_gy)], axis=0)
                for b in range(n_gx)
            ],
            axis=-1,
        )
        half = 2 * MX * MZ
        wide = 2 * xl * MZ
        part = jnp.concatenate(
            [dot(part, gx_ref[cs * half:(cs + 1) * half, :]) for cs in range(2)], axis=0
        ).reshape(2 * MY, CH // DS, DS, wide)
        value = jnp.concatenate(
            [
                dot(hy_ref[...], part[:, e].reshape(2 * MY * DS, wide).astype(BF)).reshape(yl, DS, wide)
                for e in range(CH // DS)
            ],
            axis=1,
        ).astype(BF)
        for g in range(rows_ref.shape[0]):
            rows_ref[g, :, h * CH:(h + 1) * CH] = value[:, :, g * lanes:(g + 1) * lanes]
    for h in range(halves):
        relay(h, 0).wait_send()
        loop(1, peers, lambda i: gather(h, i).wait_send())
        loop(1, peers, lambda i: relay(h, i).wait_send())


def back_kernel(
    sizes, rows_ref, pre_ref, depth_ref, gain_ref, shift_ref, out_hbm,
    out_ref, part_ref, square_ref, weigh_ref, sem,
):
    trips, G, yl, C, Z, cells, unroll = sizes
    tall, wide = cells * C, G * Z

    root = 0.5 ** 0.5
    scale = gain_ref[...] * root
    scale = 1.0 / (C * (scale * scale))
    scale = jnp.concatenate([scale] * cells, axis=-1)
    own = div(iota((8 * cells, tall), 0), 8) == div(iota((8 * cells, tall), 1), C)
    weigh_ref[...] = jnp.where(own, scale, 0.0).astype(BF)
    diagonal = iota((C, C), 0) == iota((C, C), 1)
    shift = jnp.sum(jnp.where(diagonal, shift_ref[...], 0.0), 1, keepdims=True) * root
    shift = jnp.broadcast_to(shift, (C, Z)).reshape(1, C // 8, 8, Z)

    def leave(i, slot):
        at = i * unroll * G
        return pltpu.make_async_copy(
            out_ref.at[slot], out_hbm.at[pl.ds(at, unroll * G)], sem.at[slot]
        )

    def go(i, carry):
        slot = mod(i, 2)

        @pl.when(i >= 2)
        def _():
            leave(i - 2, slot).wait()

        tiles = [(a, y) for a in range(unroll) for y in range(0, yl, cells)]

        def first(t):
            a, y = tiles[t]
            g = i * unroll + a
            part = dot(rows_ref[g, y:y + cells].reshape(tall, rows_ref.shape[-1]), depth_ref[...])
            for k in range(G):
                at = slice(k * Z, (k + 1) * Z)
                value = part[:, at] + pre_ref[g * G + k, y:y + cells].reshape(tall, Z)
                part_ref[t % 2, :, at] = value
                square_ref[t % 2, :, at] = (value * value).astype(BF)

        def second(t):
            a, y = tiles[t]
            spread = dot(weigh_ref[...], square_ref[t % 2])
            spread = lax.rsqrt(spread + norm_eps).reshape(cells, 1, 8, wide)
            for k in range(G):
                at = slice(k * Z, (k + 1) * Z)
                value = part_ref[t % 2, :, at].reshape(cells, C // 8, 8, Z)
                value = (value * spread[..., at] + shift).reshape(cells, C, Z).astype(BF)
                value = (value * root).astype(BF) * (1.0 + lax.erf(value)).astype(BF)
                out_ref[slot, a * G + k, y:y + cells] = value

        for t in range(len(tiles) + 1):
            if t < len(tiles):
                first(t)
            if t >= 1:
                second(t - 1)
        leave(i, slot).start()
        return carry

    lax.fori_loop(0, trips, go, 0)
    for i in range(max(0, trips - 2), trips):
        leave(i, i % 2).wait()


def build(mesh):
    n_gx, n_gy, n_col = (mesh.shape[a] for a in ("gx", "gy", "col"))

    def local(fields, spectral, skip_weight, skip_bias, norm_gain, norm_shift):
        hidden = fields[0]
        xl, yl, C, Z = hidden.shape
        weights = spectral[0]
        kxl, kyl, _, _, dl, MZ = weights.shape
        X, Y, MX, MY = xl * n_gx, yl * n_gy, kxl * n_gx, kyl * n_gy
        G = min(8, xl)
        steps = xl // G
        L = 2 * kxl * MZ
        n_hi = n_gy // 2
        peers = n_gx * n_hi
        G2 = min(4, xl)

        cz, sz = cos_sin(np.arange(Z), np.arange(MZ), Z)
        forward = np.concatenate([cz, -sz], axis=1)
        depth_forward = np.kron(np.eye(G), forward)
        backward = np.concatenate([cz.T, -sz.T], axis=0) / math.sqrt(MX * MY * MZ)
        depth_backward = np.kron(np.eye(G2), backward)
        cy, sy = cos_sin(np.arange(Y), signed(MY), Y)
        tyf = np.stack([cy, sy]).reshape(2, n_gy, yl, MY).transpose(1, 0, 3, 2)
        tyf = tyf.reshape(n_gy, 2 * MY, yl)
        tyi = np.stack([cy, sy]).reshape(2, n_gy, yl, MY).transpose(1, 2, 0, 3)
        tyi = tyi.reshape(n_gy, yl, 2 * MY)
        cx, sx = cos_sin(np.arange(X), signed(MX), X)
        f = np.stack([
            np.stack([np.stack([cx, -sx], 1), np.stack([sx, cx], 1)], 1),
            np.stack([np.stack([-sx, -cx], 1), np.stack([cx, -sx], 1)], 1),
        ]) / math.sqrt(X * Y * Z)
        f = f.reshape(2, n_gx, xl, 2, 2, n_gx, kxl).transpose(1, 0, 2, 3, 5, 4, 6)
        txf = f.reshape(n_gx, 4 * xl, 2 * MX)
        b = np.stack([
            np.stack([np.stack([cx, sx]), np.stack([-sx, cx])]),
            np.stack([np.stack([-sx, cx]), np.stack([-cx, -sx])]),
        ])
        b = b.reshape(2, 2, 2, n_gx, xl, n_gx, kxl).transpose(3, 0, 5, 1, 6, 4, 2)
        txi = b.reshape(n_gx, 4 * MX, 2 * xl)
        const = lambda a: jnp.asarray(a.astype(np.float32)).astype(BF)

        halves = 2 if C % 32 == 0 and n_col % 2 == 0 else 1
        CH = C // halves
        CS = 8 if CH % 8 == 0 else CH
        DS = 8 if per_dl(dl, n_col, halves) else CH
        turned = jnp.transpose(weights, (0, 1, 2, 4, 5, 3))
        tile = min(256, yl * C)

        sizes = (n_gx, n_gy, n_col, xl, yl, C, MY, MZ, kxl, kyl, dl, G, steps, halves, tile)
        tables = [const(t) for t in (depth_forward, tyf, txf, txi, tyi)]
        inside = pl.BlockSpec(memory_space=pltpu.VMEM)
        outside = pl.BlockSpec(memory_space=pltpu.HBM)
        rows_both, pre = pl.pallas_call(
            functools.partial(front_kernel, sizes),
            out_shape=(
                pltpu.VMEM((xl // G2, yl, C, G2 * 2 * MZ), BF),
                pltpu.VMEM((xl, yl, C, Z), F32),
            ),
            in_specs=[outside, outside] + [inside] * (len(tables) + 3),
            out_specs=(inside, inside),
            scratch_shapes=[
                pltpu.VMEM((xl, yl, C, Z), BF),
                pltpu.VMEM((2 * MY * CS, yl * CS), BF),
                pltpu.VMEM((4 * xl * MZ, 2 * MX * MZ), BF),
                pltpu.VMEM((2, CH // CS, yl * CS, G * 2 * MZ), BF),
                pltpu.VMEM((2, 2 * MY * CH, xl * 2 * MZ), BF),
                pltpu.VMEM((2, MY * CH, 2 * MX * MZ), F32),
                pltpu.VMEM((halves, n_hi, kyl * CH, n_gx * L), BF),
                pltpu.VMEM((halves, n_hi, kyl * CH, n_gx * L), BF),
                pltpu.VMEM((halves, n_gx, n_hi, kyl * CH, L), BF),
                pltpu.VMEM((halves, peers, kyl * CH, L), BF),
                pltpu.VMEM((kyl * C, L), BF),
                pltpu.VMEM((n_gx, n_gy, kyl * C, L), BF),
                pltpu.VMEM((4 * MX * MZ, 2 * xl * MZ), BF),
                pltpu.VMEM((yl * DS, 2 * MY * DS), BF),
                pltpu.VMEM(turned.shape, BF),
                pltpu.VMEM((n_col, kyl, dl, C, L), BF),
                pltpu.VMEM((tile, tile), BF),
                pltpu.VMEM((2 * MY, yl * CS), F32),
                pltpu.VMEM((4 * xl, 2 * MX * MZ), F32),
                pltpu.VMEM((4 * MX, 2 * xl * MZ), F32),
                pltpu.VMEM((yl, 2 * MY * DS), F32),
                pltpu.SemaphoreType.DMA((halves, steps)),
                pltpu.SemaphoreType.DMA,
                pltpu.SemaphoreType.DMA((halves,)),
                pltpu.SemaphoreType.DMA((halves,)),
                pltpu.SemaphoreType.DMA((halves, peers)),
                pltpu.SemaphoreType.DMA((halves, peers)),
                pltpu.SemaphoreType.DMA((n_col, kyl)),
                pltpu.SemaphoreType.DMA((n_col, kyl)),
                pltpu.SemaphoreType.DMA((halves, peers)),
                pltpu.SemaphoreType.DMA((halves, peers)),
                pltpu.SemaphoreType.DMA((halves, peers)),
                pltpu.SemaphoreType.DMA((halves, peers)),
            ],
            compiler_params=pltpu.CompilerParams(
                collective_id=0, has_side_effects=True, vmem_limit_bytes=40 * 2**20,
            ),
            name="front",
        )(hidden, turned, *tables, skip_weight[0], skip_bias, norm_gain)

        groups = xl // G2
        cells = min(8, yl)
        unroll = 1 if groups % 1 == 0 else 1
        out = pl.pallas_call(
            functools.partial(back_kernel, (groups // unroll, G2, yl, C, Z, cells, unroll)),
            out_shape=jax.ShapeDtypeStruct(hidden.shape, BF),
            in_specs=[inside] * 5,
            out_specs=outside,
            scratch_shapes=[
                pltpu.VMEM((2, unroll * G2, yl, C, Z), BF),
                pltpu.VMEM((2, cells * C, G2 * Z), F32),
                pltpu.VMEM((2, cells * C, G2 * Z), BF),
                pltpu.VMEM((8 * cells, cells * C), BF),
                pltpu.SemaphoreType.DMA((2,)),
            ],
            compiler_params=pltpu.CompilerParams(vmem_limit_bytes=12 * 2**20),
            name="back",
        )(rows_both, pre, const(depth_backward), norm_gain, norm_shift)
        return out[None]

    return local


def solution(mesh):
    placed = (
        P("col", "gx", "gy", None, None),
        P(None, "gx", "gy", None, None, "col", None),
        P(), P(), P(), P(),
    )
    return jax.shard_map(
        build(mesh), mesh=mesh, in_specs=placed,
        out_specs=P("col", "gx", "gy", None, None), check_vma=False,
    )
```

```python
import functools
import math

import jax
import jax.numpy as jnp
import numpy as np
from jax import lax
from jax.experimental import pallas as pl
from jax.experimental.pallas import tpu as pltpu
from jax.sharding import PartitionSpec as P

norm_eps = 1e-05
BF = jnp.bfloat16
F32 = jnp.float32
MESH = pl.DeviceIdType.MESH


def signed(count):
    index = np.arange(count)
    return np.where(index < count // 2, index, index - count)


def cos_sin(positions, frequency, length):
    turns = (positions[:, None] * frequency[None, :]) % length
    phase = turns * (2.0 * math.pi / length)
    return np.cos(phase), np.sin(phase)


def log2(n):
    assert n & (n - 1) == 0
    return n.bit_length() - 1


def div(i, n):
    return lax.shift_right_logical(i, jnp.int32(log2(n)))


def mod(i, n):
    return lax.bitwise_and(i, jnp.int32(n - 1))


def iota(shape, dim):
    return lax.broadcasted_iota(jnp.int32, shape, dim)


def dot(a, b):
    return jnp.dot(a, b, preferred_element_type=F32)


def spread_table(table, width, pick):
    r, c = table.shape
    right = (iota((c, width), 0) == pick(iota((c, width), 1))).astype(F32).astype(BF)
    return dot(table, right)


def columns(rows, width):
    tile = 256 if width % 256 == 0 else width
    return (width // tile, rows, tile)


def per_dl(dl, n_col, halves):
    return n_col == halves and dl % 8 == 0


def band(store, table_ref, rows, height, keep):
    for m in range(rows):
        store(m * height, jnp.where(keep, table_ref[m:m + 1, :], 0.0).astype(BF))


def front_kernel(
    sizes,
    fields_hbm, spectral_hbm,
    depth_hbm, tyf_hbm, txf_hbm, txi_hbm, tyi_hbm, skip_hbm, bias_hbm, gain_hbm,
    rows_ref, pre_ref,
    fields_ref, ky_ref, kx_ref, amp_ref, turn_ref, total_ref,
    swap_ref, take_ref, send_ref, recv_ref, mix_ref, modes_ref, gx_ref, hy_ref, w_ref, wa_ref,
    wbd_ref, ty_ref, tx_ref, ti_ref, th_ref,
    fsem, wsem, swap_s, swap_r, send1, recv1, send2, recv2, send3, recv3, send4, recv4,
    depth_ref, tyf_ref, txf_ref, txi_ref, tyi_ref, skip_ref, bias_ref, gain_ref, gcol_ref, tsem,
):
    n_gx, n_gy, n_col, xl, yl, C, MY, MZ, kxl, kyl, dl, G, steps, halves, tile = sizes
    n_hi = n_gy // 2
    peers = n_gx * n_hi
    MX = n_gx * kxl
    L = 2 * kxl * MZ
    CH = C // halves
    CS = 8 if CH % 8 == 0 else CH
    per = n_col // halves
    Z = fields_ref.shape[-1]
    block = kyl * CH
    top = MY * CH
    gx, gy, col = lax.axis_index("gx"), lax.axis_index("gy"), lax.axis_index("col")
    lo, hi = lax.rem(gy, 2), lax.div(gy, 2)
    mate = gy + 1 - 2 * lo
    unrolled = peers <= 16

    def peer(i):
        return lax.rem(gx + i // n_hi, n_gx), lax.rem(hi + i % n_hi, n_hi)

    def source(i):
        return lax.rem(gx + n_gx - i // n_hi, n_gx), lax.rem(hi + n_hi - i % n_hi, n_hi)

    def side(i):
        return lax.rem(col + i, n_col)

    def loop(low, high, body):
        if unrolled:
            for i in range(low, high):
                body(i)
            return

        def go(i, carry):
            body(i)
            return carry
        lax.fori_loop(low, high, go, 0)

    def field_copy(h, s):
        at = (pl.ds(s * G, G), slice(None), pl.ds(h * CH, CH), slice(None))
        return pltpu.make_async_copy(fields_hbm.at[at], fields_ref.at[at], fsem.at[h, s])

    weights_copy = pltpu.make_async_copy(spectral_hbm, w_ref, wsem)
    units = [(h, s) for h in range(halves) for s in range(steps)]
    small = [
        pltpu.make_async_copy(src, dst, tsem.at[n])
        for n, (src, dst) in enumerate((
            (tyf_hbm.at[gy], tyf_ref), (txf_hbm.at[gx], txf_ref), (depth_hbm, depth_ref),
            (txi_hbm.at[gx], txi_ref), (tyi_hbm.at[gy], tyi_ref), (skip_hbm, skip_ref),
            (bias_hbm, bias_ref), (gain_hbm, gain_ref),
        ))
    ]
    for copy in small[:2]:
        copy.start()
    weights_copy.start()
    small[2].start()
    for unit in units[:3]:
        field_copy(*unit).start()
    for copy in small[3:]:
        copy.start()

    barrier = pltpu.get_barrier_semaphore()

    def greet(i):
        px, ph = peer(i)
        pl.semaphore_signal(
            barrier, inc=1, device_id={"gx": px, "gy": 2 * ph + lo}, device_id_type=MESH
        )

    def greet_side(i):
        pl.semaphore_signal(barrier, inc=1, device_id={"col": side(i)}, device_id_type=MESH)

    loop(1, peers, greet)
    loop(1, n_col, greet_side)
    pl.semaphore_signal(barrier, inc=1, device_id={"gy": mate}, device_id_type=MESH)

    for copy in small[:2]:
        copy.wait()
    ty_ref[...] = spread_table(tyf_ref[...], yl * CS, lambda j: div(j, CS))
    tx_ref[...] = spread_table(txf_ref[...], 2 * MX * MZ, lambda j: div(j, MZ))

    def put_ky(first, value):
        ky_ref[pl.ds(first, CS), :] = value

    band(put_ky, ty_ref, 2 * MY, CS, iota((CS, yl * CS), 0) == mod(iota((CS, yl * CS), 1), CS))

    def put_kx(first, value):
        for n in range(kx_ref.shape[0]):
            kx_ref[n, pl.ds(first, MZ), :] = value[:, n * kx_ref.shape[2]:(n + 1) * kx_ref.shape[2]]

    wide = 2 * MX * MZ
    band(put_kx, tx_ref, 4 * steps * G, MZ, iota((MZ, wide), 0) == mod(iota((MZ, wide), 1), MZ))

    def share(i, k):
        return pltpu.make_async_remote_copy(
            src_ref=wa_ref.at[col, k], dst_ref=wa_ref.at[col, k],
            send_sem=send2.at[i, k], recv_sem=recv2.at[i, k],
            device_id={"col": side(i)}, device_id_type=MESH,
        )

    def swap(h):
        return pltpu.make_async_remote_copy(
            src_ref=swap_ref.at[h], dst_ref=take_ref.at[h],
            send_sem=swap_s.at[h], recv_sem=swap_r.at[h],
            device_id={"gy": mate}, device_id_type=MESH,
        )

    def scatter(h, i):
        px, ph = peer(i)
        return pltpu.make_async_remote_copy(
            src_ref=send_ref.at[h, px, ph], dst_ref=recv_ref.at[h, i],
            send_sem=send1.at[h, i], recv_sem=recv1.at[h, i],
            device_id={"gx": px, "gy": 2 * ph + lo}, device_id_type=MESH,
        )

    span = kyl * C // halves
    each = n_col // halves

    def gather(h, i):
        px, ph = peer(i)
        cut = pl.ds(h * each, each)
        return pltpu.make_async_remote_copy(
            src_ref=mix_ref.at[cut], dst_ref=modes_ref.at[gx, gy, cut],
            send_sem=send3.at[h, i], recv_sem=recv3.at[h, i],
            device_id={"gx": px, "gy": 2 * ph + lo}, device_id_type=MESH,
        )

    def relay(h, i):
        cut = pl.ds(h * each, each)
        if isinstance(i, int) and i == 0:
            src, at = mix_ref.at[cut], modes_ref.at[gx, gy, cut]
        else:
            sx, sh = source(i)
            src = at = modes_ref.at[sx, 2 * sh + lo, cut]
        return pltpu.make_async_remote_copy(
            src_ref=src, dst_ref=at, send_sem=send4.at[h, i], recv_sem=recv4.at[h, i],
            device_id={"gy": mate}, device_id_type=MESH,
        )

    def prepare_weights():
        weights_copy.wait()
        eye = (iota((C, C), 0) == iota((C, C), 1)).astype(F32).astype(BF)
        for k in range(kyl):
            for d in range(dl):
                parts = [w_ref[j, k, r, d] for r in range(2) for j in range(kxl)]
                wa_ref[col, k, d] = lax.dot_general(
                    eye, jnp.concatenate(parts, axis=0), (((1,), (1,)), ((), ())),
                    preferred_element_type=F32,
                ).astype(BF)
            if k == 0:
                pl.semaphore_wait(barrier, peers + n_col - 1)
            for i in range(1, n_col):
                share(i, k).start()

    def z_stage(u):
        h, s = units[u]
        field_copy(h, s).wait()
        if u + 3 < len(units):
            field_copy(*units[u + 3]).start()
        lhs = jnp.concatenate(
            [fields_ref[s * G + g, :, h * CH:(h + 1) * CH, :].reshape(yl * CH, Z) for g in range(G)],
            axis=-1,
        )
        rows = yl // 2
        for f in range(2):
            value = dot(lhs[f * rows * CH:(f + 1) * rows * CH], depth_ref[...])
            value = value.reshape(rows, CH // CS, CS, 2 * G * MZ)
            for e in range(CH // CS):
                amp_ref[u % 2, e, f * rows * CS:(f + 1) * rows * CS] = value[:, e].reshape(
                    rows * CS, 2 * G * MZ
                ).astype(BF)

    def y_stage(u):
        h, s = units[u]
        lanes = 2 * G * MZ
        value = jnp.concatenate(
            [
                dot(ky_ref[...], amp_ref[u % 2, e]).reshape(2 * MY, CS, lanes)
                for e in range(CH // CS)
            ],
            axis=1,
        )
        turn_ref[h % 2, s] = value.reshape(2 * MY * CH, lanes).astype(BF)

    def joined(ref, low, high):
        return jnp.concatenate([ref[n, low:high] for n in range(ref.shape[0])], axis=-1)

    def x_stage(u):
        h, s = units[u]
        lanes = 2 * G * MZ
        term = dot(turn_ref[h % 2, s, :top], joined(kx_ref, s * lanes, (s + 1) * lanes))
        later = (steps + s) * lanes
        term = term + dot(turn_ref[h % 2, s, top:], joined(kx_ref, later, later + lanes))
        for b in range(n_gx):
            if s == 0:
                total_ref[h % 2, b] = term[:, b * L:(b + 1) * L]
            else:
                total_ref[h % 2, b] += term[:, b * L:(b + 1) * L]
        if s == steps - 1:
            for i in range(n_hi):
                at = pl.multiple_of((2 * i + 1 - lo) * block, block)
                for b in range(n_gx):
                    swap_ref[h, i, b] = total_ref[h % 2, b, pl.ds(at, block), :].astype(BF)
            swap(h).start()

    def send_half(h):
        swap(h).wait_recv()
        for i in range(n_hi):
            at = pl.multiple_of((2 * i + lo) * block, block)
            for b in range(n_gx):
                value = total_ref[h % 2, b, pl.ds(at, block), :] + take_ref[h, i, b].astype(F32)
                send_ref[h, b, i] = value.astype(BF)
        loop(1, peers, lambda i: scatter(h, i).start())

    prepare_weights()
    small[2].wait()
    for u in range(len(units) + 1):
        if u < len(units):
            z_stage(u)
        if 0 <= u - 1:
            y_stage(u - 1)
            x_stage(u - 1)
        if halves > 1 and u == steps + 1:
            send_half(0)

    for copy in small[3:]:
        copy.wait()
    weight = skip_ref[...].astype(F32)
    weight = (weight - jnp.mean(weight, axis=0, keepdims=True)).astype(BF)
    tall = spread_table(weight, tile, lambda j: mod(j, C))
    for g in range(tile // C):
        keep = div(iota((C, tile), 1), C) == g
        wbd_ref[g * C:(g + 1) * C, :] = jnp.where(keep, tall, 0.0).astype(BF)
    diagonal = iota((C, C), 0) == iota((C, C), 1)
    bias = jnp.sum(jnp.where(diagonal, bias_ref[...], 0.0), 1, keepdims=True)
    gain = jnp.sum(jnp.where(diagonal, gain_ref[...], 0.0), 1, keepdims=True) * (0.5 ** 0.5)
    for q in range(n_col):
        gcol_ref[q] = jnp.broadcast_to(gain[q * dl:(q + 1) * dl], (dl, L))
    bias = ((bias - jnp.mean(bias, axis=0, keepdims=True)) * gain)[None]

    def skip_cells(low, high):
        def go(i, carry):
            x = 2 * i
            for y in range(0, yl, tile // C):
                hidden = jnp.concatenate(
                    [fields_ref[x + k, y:y + tile // C].reshape(tile, Z) for k in range(2)], axis=-1
                )
                part = dot(wbd_ref[...], hidden).reshape(tile // C, C, 2 * Z) * gain[None] + bias
                for k in range(2):
                    pre_ref[x + k, y:y + tile // C] = part[:, :, k * Z:(k + 1) * Z]
            return carry
        lax.fori_loop(low, high, go, 0)

    pairs = xl // 2
    early, mid = pairs // 8, pairs // 2
    skip_cells(0, early)
    send_half(halves - 1)

    ti_ref[...] = spread_table(txi_ref[...], 2 * xl * MZ, lambda j: div(j, MZ))
    DS = 8 if per_dl(dl, n_col, halves) else CH
    th_ref[...] = spread_table(
        tyi_ref[...], 2 * MY * DS,
        (lambda j: div(j, DS)) if DS < CH else
        (lambda j: div(j, per * kyl * dl) * kyl + mod(div(j, dl), kyl)),
    )

    def put_gx(first, value):
        for n in range(gx_ref.shape[0]):
            gx_ref[n, pl.ds(first, MZ), :] = value[:, n * gx_ref.shape[2]:(n + 1) * gx_ref.shape[2]]

    wide = 2 * xl * MZ
    band(put_gx, ti_ref, 4 * MX, MZ, iota((MZ, wide), 0) == mod(iota((MZ, wide), 1), MZ))

    def put_hy(first, value):
        hy_ref[pl.ds(first, DS), :] = value

    j = iota((DS, 2 * MY * DS), 1)
    chan = mod(j, DS) if DS < CH else mod(div(j, kyl * dl), per) * dl + mod(j, dl)
    band(put_hy, th_ref, yl, DS, iota((DS, 2 * MY * DS), 0) == chan)
    skip_cells(early, early + mid)

    sums = {}
    for h in range(halves):
        total = send_ref[h, gx, hi].astype(F32)
        for i in range(1, peers):
            scatter(h, i).wait_recv()
            total = total + recv_ref[h, i].astype(F32)
        spec = total.astype(BF).astype(F32)
        re, im = spec[:, :L // 2], spec[:, L // 2:]
        re = jnp.concatenate([re, re], axis=-1)
        im = jnp.concatenate([im, im], axis=-1)
        for a in range(n_col):
            for k in range(kyl):
                if h == 0 and a > 0:
                    share(n_col - a, k).wait_recv()
                rows, chans = slice(k * CH, (k + 1) * CH), slice(h * CH, (h + 1) * CH)
                weight = wa_ref[side(a), k, :, chans].astype(F32)
                new = [jnp.sum(v[rows][None] * weight, axis=1) for v in (re, im)]
                old = sums.get((a, k))
                sums[a, k] = new if old is None else [x + y for x, y in zip(old, new)]
    for k in range(kyl):
        mixed = []
        for a in range(n_col):
            first, second = sums[a, k]
            turned_second = jnp.concatenate(
                [-second[:, L // 2:], second[:, :L // 2]], axis=-1
            )
            mixed.append(first + turned_second)
        centre = sum(jnp.sum(m, axis=0, keepdims=True) for m in mixed) * (1.0 / C)
        for a in range(n_col):
            mix_ref[side(a), k] = ((mixed[a] - centre) * gcol_ref[side(a)]).astype(BF)

    def send_modes(h):
        loop(1, peers, lambda i: gather(h, i).start())
        relay(h, 0).start()

    def sent_modes(h):
        loop(1, peers, lambda i: gather(h, i).wait_send())
        relay(h, 0).wait_send()

    send_modes(0)
    modes_ref[gx, gy] = mix_ref[...]
    skip_cells(early + mid, pairs)
    for h in range(1, halves):
        sent_modes(h - 1)
        send_modes(h)
    for h in range(halves):
        swap(h).wait_send()
        loop(1, peers, lambda i: scatter(h, i).wait_send())
    for i in range(1, n_col):
        for k in range(kyl):
            share(i, k).wait_send()

    lanes = rows_ref.shape[-1]
    for h in range(halves):
        def pass_on(i):
            gather(h, i).wait_recv()
            relay(h, i).start()

        loop(1, peers, pass_on)
        relay(h, 0).wait_recv()
        loop(1, peers, lambda i: relay(h, i).wait_recv())
        part = jnp.concatenate(
            [
                jnp.concatenate([modes_ref[b, g, h * each:(h + 1) * each].reshape(span, L) for g in range(n_gy)], axis=0)
                for b in range(n_gx)
            ],
            axis=-1,
        )
        half = 2 * MX * MZ
        wide = 2 * xl * MZ
        part = jnp.concatenate(
            [dot(part, joined(gx_ref, cs * half, (cs + 1) * half)) for cs in range(2)], axis=0
        ).reshape(2 * MY, CH // DS, DS, wide)
        value = jnp.concatenate(
            [
                dot(hy_ref[...], part[:, e].reshape(2 * MY * DS, wide).astype(BF)).reshape(yl, DS, wide)
                for e in range(CH // DS)
            ],
            axis=1,
        ).astype(BF)
        for g in range(rows_ref.shape[0]):
            rows_ref[g, :, h * CH:(h + 1) * CH] = value[:, :, g * lanes:(g + 1) * lanes]
    sent_modes(halves - 1)
    for h in range(halves):
        loop(1, peers, lambda i: relay(h, i).wait_send())


def back_kernel(
    sizes, rows_ref, pre_ref, depth_ref, gain_ref, shift_ref, out_hbm,
    out_ref, part_ref, square_ref, weigh_ref, sem,
):
    trips, G, yl, C, Z, cells, unroll = sizes
    tall, wide = cells * C, G * Z

    root = 0.5 ** 0.5
    scale = gain_ref[...] * root
    scale = 1.0 / (C * (scale * scale))
    scale = jnp.concatenate([scale] * cells, axis=-1)
    own = div(iota((8 * cells, tall), 0), 8) == div(iota((8 * cells, tall), 1), C)
    weigh_ref[...] = jnp.where(own, scale, 0.0).astype(BF)
    diagonal = iota((C, C), 0) == iota((C, C), 1)
    shift = jnp.sum(jnp.where(diagonal, shift_ref[...], 0.0), 1, keepdims=True) * root
    shift = jnp.broadcast_to(shift, (C, Z)).reshape(1, C // 8, 8, Z)

    def leave(i, slot):
        at = i * unroll * G
        return pltpu.make_async_copy(
            out_ref.at[slot], out_hbm.at[pl.ds(at, unroll * G)], sem.at[slot]
        )

    def go(i, carry):
        slot = mod(i, 2)

        @pl.when(i >= 2)
        def _():
            leave(i - 2, slot).wait()

        tiles = [(a, y) for a in range(unroll) for y in range(0, yl, cells)]

        def first(t):
            a, y = tiles[t]
            g = i * unroll + a
            part = dot(rows_ref[g, y:y + cells].reshape(tall, rows_ref.shape[-1]), depth_ref[...])
            for k in range(G):
                at = slice(k * Z, (k + 1) * Z)
                value = part[:, at] + pre_ref[g * G + k, y:y + cells].reshape(tall, Z)
                part_ref[t % 2, k] = value
                square_ref[t % 2, k] = (value * value).astype(BF)

        def second(t):
            a, y = tiles[t]
            square = jnp.concatenate([square_ref[t % 2, k] for k in range(G)], axis=-1)
            spread = dot(weigh_ref[...], square)
            spread = lax.rsqrt(spread + norm_eps).reshape(cells, 1, 8, wide)
            for k in range(G):
                at = slice(k * Z, (k + 1) * Z)
                value = part_ref[t % 2, k].reshape(cells, C // 8, 8, Z)
                value = (value * spread[..., at] + shift).reshape(cells, C, Z).astype(BF)
                value = (value * root).astype(BF) * (1.0 + lax.erf(value)).astype(BF)
                out_ref[slot, a * G + k, y:y + cells] = value

        for t in range(len(tiles) + 1):
            if t < len(tiles):
                first(t)
            if t >= 1:
                second(t - 1)
        leave(i, slot).start()
        return carry

    lax.fori_loop(0, trips, go, 0)
    for i in range(max(0, trips - 2), trips):
        leave(i, i % 2).wait()


def build(mesh):
    n_gx, n_gy, n_col = (mesh.shape[a] for a in ("gx", "gy", "col"))

    def local(fields, spectral, skip_weight, skip_bias, norm_gain, norm_shift):
        hidden = fields[0]
        xl, yl, C, Z = hidden.shape
        weights = spectral[0]
        kxl, kyl, _, _, dl, MZ = weights.shape
        X, Y, MX, MY = xl * n_gx, yl * n_gy, kxl * n_gx, kyl * n_gy
        G = min(8, xl)
        steps = xl // G
        L = 2 * kxl * MZ
        n_hi = n_gy // 2
        peers = n_gx * n_hi
        G2 = min(4, xl)

        cz, sz = cos_sin(np.arange(Z), np.arange(MZ), Z)
        forward = np.concatenate([cz, -sz], axis=1)
        depth_forward = np.kron(np.eye(G), forward)
        backward = np.concatenate([cz.T, -sz.T], axis=0) / math.sqrt(MX * MY * MZ)
        depth_backward = np.kron(np.eye(G2), backward)
        cy, sy = cos_sin(np.arange(Y), signed(MY), Y)
        tyf = np.stack([cy, sy]).reshape(2, n_gy, yl, MY).transpose(1, 0, 3, 2)
        tyf = tyf.reshape(n_gy, 2 * MY, yl)
        tyi = np.stack([cy, sy]).reshape(2, n_gy, yl, MY).transpose(1, 2, 0, 3)
        tyi = tyi.reshape(n_gy, yl, 2 * MY)
        cx, sx = cos_sin(np.arange(X), signed(MX), X)
        f = np.stack([
            np.stack([np.stack([cx, -sx], 1), np.stack([sx, cx], 1)], 1),
            np.stack([np.stack([-sx, -cx], 1), np.stack([cx, -sx], 1)], 1),
        ]) / math.sqrt(X * Y * Z)
        f = f.reshape(2, n_gx, xl, 2, 2, n_gx, kxl).transpose(1, 0, 2, 3, 5, 4, 6)
        txf = f.reshape(n_gx, 4 * xl, 2 * MX)
        b = np.stack([
            np.stack([np.stack([cx, sx]), np.stack([-sx, cx])]),
            np.stack([np.stack([-sx, cx]), np.stack([-cx, -sx])]),
        ])
        b = b.reshape(2, 2, 2, n_gx, xl, n_gx, kxl).transpose(3, 0, 5, 1, 6, 4, 2)
        txi = b.reshape(n_gx, 4 * MX, 2 * xl)
        const = lambda a: jnp.asarray(a.astype(np.float32)).astype(BF)

        halves = 2 if C % 32 == 0 and n_col % 2 == 0 else 1
        CH = C // halves
        CS = 8 if CH % 8 == 0 else CH
        DS = 8 if per_dl(dl, n_col, halves) else CH
        turned = jnp.transpose(weights, (0, 1, 2, 4, 5, 3))
        tile = min(256, yl * C)

        sizes = (n_gx, n_gy, n_col, xl, yl, C, MY, MZ, kxl, kyl, dl, G, steps, halves, tile)
        tables = [const(t) for t in (depth_forward, tyf, txf, txi, tyi)]
        inside = pl.BlockSpec(memory_space=pltpu.VMEM)
        outside = pl.BlockSpec(memory_space=pltpu.HBM)
        rows_both, pre = pl.pallas_call(
            functools.partial(front_kernel, sizes),
            out_shape=(
                pltpu.VMEM((xl // G2, yl, C, G2 * 2 * MZ), BF),
                pltpu.VMEM((xl, yl, C, Z), F32),
            ),
            in_specs=[outside] * (len(tables) + 5),
            out_specs=(inside, inside),
            scratch_shapes=[
                pltpu.VMEM((xl, yl, C, Z), BF),
                pltpu.VMEM((2 * MY * CS, yl * CS), BF),
                pltpu.VMEM(columns(4 * xl * MZ, 2 * MX * MZ), BF),
                pltpu.VMEM((2, CH // CS, yl * CS, G * 2 * MZ), BF),
                pltpu.VMEM((2, steps, 2 * MY * CH, G * 2 * MZ), BF),
                pltpu.VMEM((2, n_gx, MY * CH, L), F32),
                pltpu.VMEM((halves, n_hi, n_gx, kyl * CH, L), BF),
                pltpu.VMEM((halves, n_hi, n_gx, kyl * CH, L), BF),
                pltpu.VMEM((halves, n_gx, n_hi, kyl * CH, L), BF),
                pltpu.VMEM((halves, peers, kyl * CH, L), BF),
                pltpu.VMEM((n_col, kyl, dl, L), BF),
                pltpu.VMEM((n_gx, n_gy, n_col, kyl, dl, L), BF),
                pltpu.VMEM(columns(4 * MX * MZ, 2 * xl * MZ), BF),
                pltpu.VMEM((yl * DS, 2 * MY * DS), BF),
                pltpu.VMEM(turned.shape, BF),
                pltpu.VMEM((n_col, kyl, dl, C, L), BF),
                pltpu.VMEM((tile, tile), BF),
                pltpu.VMEM((2 * MY, yl * CS), F32),
                pltpu.VMEM((4 * xl, 2 * MX * MZ), F32),
                pltpu.VMEM((4 * MX, 2 * xl * MZ), F32),
                pltpu.VMEM((yl, 2 * MY * DS), F32),
                pltpu.SemaphoreType.DMA((halves, steps)),
                pltpu.SemaphoreType.DMA,
                pltpu.SemaphoreType.DMA((halves,)),
                pltpu.SemaphoreType.DMA((halves,)),
                pltpu.SemaphoreType.DMA((halves, peers)),
                pltpu.SemaphoreType.DMA((halves, peers)),
                pltpu.SemaphoreType.DMA((n_col, kyl)),
                pltpu.SemaphoreType.DMA((n_col, kyl)),
                pltpu.SemaphoreType.DMA((halves, peers)),
                pltpu.SemaphoreType.DMA((halves, peers)),
                pltpu.SemaphoreType.DMA((halves, peers)),
                pltpu.SemaphoreType.DMA((halves, peers)),
                pltpu.VMEM(tables[0].shape, BF),
                pltpu.VMEM(tables[1].shape[1:], BF),
                pltpu.VMEM(tables[2].shape[1:], BF),
                pltpu.VMEM(tables[3].shape[1:], BF),
                pltpu.VMEM(tables[4].shape[1:], BF),
                pltpu.VMEM((C, C), BF),
                pltpu.VMEM((1, C), F32),
                pltpu.VMEM((1, C), F32),
                pltpu.VMEM((n_col, dl, L), F32),
                pltpu.SemaphoreType.DMA((8,)),
            ],
            compiler_params=pltpu.CompilerParams(
                collective_id=0, has_side_effects=True, vmem_limit_bytes=40 * 2**20,
            ),
            name="front",
        )(hidden, turned, *tables, skip_weight[0], skip_bias, norm_gain)

        groups = xl // G2
        cells = min(8, yl)
        unroll = 1 if groups % 1 == 0 else 1
        out = pl.pallas_call(
            functools.partial(back_kernel, (groups // unroll, G2, yl, C, Z, cells, unroll)),
            out_shape=jax.ShapeDtypeStruct(hidden.shape, BF),
            in_specs=[inside] * 5,
            out_specs=outside,
            scratch_shapes=[
                pltpu.VMEM((2, unroll * G2, yl, C, Z), BF),
                pltpu.VMEM((2, G2, cells * C, Z), F32),
                pltpu.VMEM((2, G2, cells * C, Z), BF),
                pltpu.VMEM((8 * cells, cells * C), BF),
                pltpu.SemaphoreType.DMA((2,)),
            ],
            compiler_params=pltpu.CompilerParams(vmem_limit_bytes=12 * 2**20),
            name="back",
        )(rows_both, pre, const(depth_backward), norm_gain, norm_shift)
        return out[None]

    return local


def solution(mesh):
    placed = (
        P("col", "gx", "gy", None, None),
        P(None, "gx", "gy", None, None, "col", None),
        P(), P(), P(), P(),
    )
    return jax.shard_map(
        build(mesh), mesh=mesh, in_specs=placed,
        out_specs=P("col", "gx", "gy", None, None), check_vma=False,
    )
```

```python
import functools
import math

import jax
import jax.numpy as jnp
import numpy as np
from jax import lax
from jax.experimental import pallas as pl
from jax.experimental.pallas import tpu as pltpu
from jax.sharding import PartitionSpec as P

norm_eps = 1e-05
BF = jnp.bfloat16
F32 = jnp.float32
MESH = pl.DeviceIdType.MESH


def signed(count):
    index = np.arange(count)
    return np.where(index < count // 2, index, index - count)


def cos_sin(positions, frequency, length):
    turns = (positions[:, None] * frequency[None, :]) % length
    phase = turns * (2.0 * math.pi / length)
    return np.cos(phase), np.sin(phase)


def log2(n):
    assert n & (n - 1) == 0
    return n.bit_length() - 1


def div(i, n):
    return lax.shift_right_logical(i, jnp.int32(log2(n)))


def mod(i, n):
    return lax.bitwise_and(i, jnp.int32(n - 1))


def iota(shape, dim):
    return lax.broadcasted_iota(jnp.int32, shape, dim)


def dot(a, b):
    return jnp.dot(a, b, preferred_element_type=F32)


def spread_table(table, width, pick):
    r, c = table.shape
    right = (iota((c, width), 0) == pick(iota((c, width), 1))).astype(F32).astype(BF)
    return dot(table, right)


def columns(rows, width):
    tile = 256 if width % 256 == 0 else width
    return (width // tile, rows, tile)


def per_dl(dl, n_col, halves):
    return n_col == halves and dl % 8 == 0


def band(store, table_ref, rows, height, keep):
    for m in range(rows):
        store(m * height, jnp.where(keep, table_ref[m:m + 1, :], 0.0).astype(BF))


def front_kernel(
    sizes,
    fields_hbm, spectral_hbm,
    depth_hbm, tyf_hbm, txf_hbm, txi_hbm, tyi_hbm, skip_hbm, bias_hbm, gain_hbm,
    rows_ref, pre_ref,
    fields_ref, ky_ref, kx_ref, amp_ref, turn_ref, total_ref,
    swap_ref, take_ref, send_ref, recv_ref, mix_ref, modes_ref, gx_ref, hy_ref, w_ref, wa_ref,
    wbd_ref, ty_ref, tx_ref, ti_ref, th_ref,
    fsem, wsem, swap_s, swap_r, send1, recv1, send2, recv2, send3, recv3, send4, recv4,
    depth_ref, tyf_ref, txf_ref, txi_ref, tyi_ref, skip_ref, bias_ref, gain_ref, gcol_ref, tsem,
):
    n_gx, n_gy, n_col, xl, yl, C, MY, MZ, kxl, kyl, dl, G, steps, halves, tile = sizes
    n_hi = n_gy // 2
    peers = n_gx * n_hi
    MX = n_gx * kxl
    L = 2 * kxl * MZ
    CH = C // halves
    CS = 8 if CH % 8 == 0 else CH
    per = n_col // halves
    Z = fields_ref.shape[-1]
    block = kyl * CH
    top = MY * CH
    gx, gy, col = lax.axis_index("gx"), lax.axis_index("gy"), lax.axis_index("col")
    lo, hi = lax.rem(gy, 2), lax.div(gy, 2)
    mate = gy + 1 - 2 * lo
    unrolled = peers <= 16

    def peer(i):
        return lax.rem(gx + i // n_hi, n_gx), lax.rem(hi + i % n_hi, n_hi)

    def source(i):
        return lax.rem(gx + n_gx - i // n_hi, n_gx), lax.rem(hi + n_hi - i % n_hi, n_hi)

    def side(i):
        return lax.rem(col + i, n_col)

    def loop(low, high, body):
        if unrolled:
            for i in range(low, high):
                body(i)
            return

        def go(i, carry):
            body(i)
            return carry
        lax.fori_loop(low, high, go, 0)

    def field_copy(h, s):
        at = (pl.ds(s * G, G), slice(None), pl.ds(h * CH, CH), slice(None))
        return pltpu.make_async_copy(fields_hbm.at[at], fields_ref.at[at], fsem.at[h, s])

    weights_copy = pltpu.make_async_copy(spectral_hbm, w_ref, wsem)
    units = [(h, s) for h in range(halves) for s in range(steps)]
    small = [
        pltpu.make_async_copy(src, dst, tsem.at[n])
        for n, (src, dst) in enumerate((
            (tyf_hbm.at[gy], tyf_ref), (txf_hbm.at[gx], txf_ref), (depth_hbm, depth_ref),
            (txi_hbm.at[gx], txi_ref), (tyi_hbm.at[gy], tyi_ref), (skip_hbm, skip_ref),
            (bias_hbm, bias_ref), (gain_hbm, gain_ref),
        ))
    ]
    for copy in small[:2]:
        copy.start()
    weights_copy.start()
    small[2].start()
    for unit in units[:3]:
        field_copy(*unit).start()
    for copy in small[3:]:
        copy.start()

    barrier = pltpu.get_barrier_semaphore()

    def greet(i):
        px, ph = peer(i)
        pl.semaphore_signal(
            barrier, inc=1, device_id={"gx": px, "gy": 2 * ph + lo}, device_id_type=MESH
        )

    def greet_side(i):
        pl.semaphore_signal(barrier, inc=1, device_id={"col": side(i)}, device_id_type=MESH)

    loop(1, peers, greet)
    loop(1, n_col, greet_side)
    pl.semaphore_signal(barrier, inc=1, device_id={"gy": mate}, device_id_type=MESH)

    for copy in small[:2]:
        copy.wait()
    ty_ref[...] = spread_table(tyf_ref[...], yl * CS, lambda j: div(j, CS))
    tx_ref[...] = spread_table(txf_ref[...], 2 * MX * MZ, lambda j: div(j, MZ))

    def put_ky(first, value):
        ky_ref[pl.ds(first, CS), :] = value

    band(put_ky, ty_ref, 2 * MY, CS, iota((CS, yl * CS), 0) == mod(iota((CS, yl * CS), 1), CS))

    def put_kx(first, value):
        for n in range(kx_ref.shape[0]):
            kx_ref[n, pl.ds(first, MZ), :] = value[:, n * kx_ref.shape[2]:(n + 1) * kx_ref.shape[2]]

    wide = 2 * MX * MZ
    band(put_kx, tx_ref, 4 * steps * G, MZ, iota((MZ, wide), 0) == mod(iota((MZ, wide), 1), MZ))

    def share(i, k):
        return pltpu.make_async_remote_copy(
            src_ref=wa_ref.at[col, k], dst_ref=wa_ref.at[col, k],
            send_sem=send2.at[i, k], recv_sem=recv2.at[i, k],
            device_id={"col": side(i)}, device_id_type=MESH,
        )

    def swap(h):
        return pltpu.make_async_remote_copy(
            src_ref=swap_ref.at[h], dst_ref=take_ref.at[h],
            send_sem=swap_s.at[h], recv_sem=swap_r.at[h],
            device_id={"gy": mate}, device_id_type=MESH,
        )

    def scatter(h, i):
        px, ph = peer(i)
        return pltpu.make_async_remote_copy(
            src_ref=send_ref.at[h, px, ph], dst_ref=recv_ref.at[h, i],
            send_sem=send1.at[h, i], recv_sem=recv1.at[h, i],
            device_id={"gx": px, "gy": 2 * ph + lo}, device_id_type=MESH,
        )

    span = kyl * C // halves
    each = n_col // halves

    def gather(h, i):
        px, ph = peer(i)
        cut = pl.ds(h * each, each)
        return pltpu.make_async_remote_copy(
            src_ref=mix_ref.at[cut], dst_ref=modes_ref.at[gx, gy, cut],
            send_sem=send3.at[h, i], recv_sem=recv3.at[h, i],
            device_id={"gx": px, "gy": 2 * ph + lo}, device_id_type=MESH,
        )

    def relay(h, i):
        cut = pl.ds(h * each, each)
        if isinstance(i, int) and i == 0:
            src, at = mix_ref.at[cut], modes_ref.at[gx, gy, cut]
        else:
            sx, sh = source(i)
            src = at = modes_ref.at[sx, 2 * sh + lo, cut]
        return pltpu.make_async_remote_copy(
            src_ref=src, dst_ref=at, send_sem=send4.at[h, i], recv_sem=recv4.at[h, i],
            device_id={"gy": mate}, device_id_type=MESH,
        )

    def prepare_weights():
        weights_copy.wait()
        eye = (iota((C, C), 0) == iota((C, C), 1)).astype(F32).astype(BF)
        for k in range(kyl):
            for d in range(dl):
                parts = [w_ref[j, k, r, d] for r in range(2) for j in range(kxl)]
                wa_ref[col, k, d] = lax.dot_general(
                    eye, jnp.concatenate(parts, axis=0), (((1,), (1,)), ((), ())),
                    preferred_element_type=F32,
                ).astype(BF)
            if k == 0:
                pl.semaphore_wait(barrier, peers + n_col - 1)
            for i in range(1, n_col):
                share(i, k).start()

    def z_stage(u):
        h, s = units[u]
        field_copy(h, s).wait()
        if u + 3 < len(units):
            field_copy(*units[u + 3]).start()
        lhs = jnp.concatenate(
            [fields_ref[s * G + g, :, h * CH:(h + 1) * CH, :].reshape(yl * CH, Z) for g in range(G)],
            axis=-1,
        )
        rows = yl // 2
        for f in range(2):
            value = dot(lhs[f * rows * CH:(f + 1) * rows * CH], depth_ref[...])
            value = value.reshape(rows, CH // CS, CS, 2 * G * MZ)
            for e in range(CH // CS):
                amp_ref[u % 2, e, f * rows * CS:(f + 1) * rows * CS] = value[:, e].reshape(
                    rows * CS, 2 * G * MZ
                ).astype(BF)

    def y_stage(u):
        h, s = units[u]
        lanes = 2 * G * MZ
        value = jnp.concatenate(
            [
                dot(ky_ref[...], amp_ref[u % 2, e]).reshape(2 * MY, CS, lanes)
                for e in range(CH // CS)
            ],
            axis=1,
        )
        turn_ref[h % 2, s] = value.reshape(2 * MY * CH, lanes).astype(BF)

    def joined(ref, low, high):
        return jnp.concatenate([ref[n, low:high] for n in range(ref.shape[0])], axis=-1)

    def x_stage(u):
        h, s = units[u]
        lanes = 2 * G * MZ
        term = dot(turn_ref[h % 2, s, :top], joined(kx_ref, s * lanes, (s + 1) * lanes))
        later = (steps + s) * lanes
        term = term + dot(turn_ref[h % 2, s, top:], joined(kx_ref, later, later + lanes))
        for b in range(n_gx):
            if s == 0:
                total_ref[h % 2, b] = term[:, b * L:(b + 1) * L]
            else:
                total_ref[h % 2, b] += term[:, b * L:(b + 1) * L]
        if s == steps - 1:
            for i in range(n_hi):
                at = pl.multiple_of((2 * i + 1 - lo) * block, block)
                for b in range(n_gx):
                    swap_ref[h, i, b] = total_ref[h % 2, b, pl.ds(at, block), :].astype(BF)
            swap(h).start()

    def send_half(h):
        swap(h).wait_recv()
        for i in range(n_hi):
            at = pl.multiple_of((2 * i + lo) * block, block)
            for b in range(n_gx):
                value = total_ref[h % 2, b, pl.ds(at, block), :] + take_ref[h, i, b].astype(F32)
                send_ref[h, b, i] = value.astype(BF)
        loop(1, peers, lambda i: scatter(h, i).start())

    prepare_weights()
    small[2].wait()
    for u in range(len(units) + 1):
        if u < len(units):
            z_stage(u)
        if 0 <= u - 1:
            y_stage(u - 1)
            x_stage(u - 1)
        if halves > 1 and u == steps + 1:
            send_half(0)

    for copy in small[3:]:
        copy.wait()
    weight = skip_ref[...].astype(F32)
    weight = (weight - jnp.mean(weight, axis=0, keepdims=True)).astype(BF)
    tall = spread_table(weight, tile, lambda j: mod(j, C))
    for g in range(tile // C):
        keep = div(iota((C, tile), 1), C) == g
        wbd_ref[g * C:(g + 1) * C, :] = jnp.where(keep, tall, 0.0).astype(BF)
    diagonal = iota((C, C), 0) == iota((C, C), 1)
    bias = jnp.sum(jnp.where(diagonal, bias_ref[...], 0.0), 1, keepdims=True)
    gain = jnp.sum(jnp.where(diagonal, gain_ref[...], 0.0), 1, keepdims=True) * (0.5 ** 0.5)
    for q in range(n_col):
        gcol_ref[q] = jnp.broadcast_to(gain[q * dl:(q + 1) * dl], (dl, L))
    bias = ((bias - jnp.mean(bias, axis=0, keepdims=True)) * gain)[None]

    def skip_cells(low, high):
        def go(i, carry):
            x = 2 * i
            for y in range(0, yl, tile // C):
                hidden = jnp.concatenate(
                    [fields_ref[x + k, y:y + tile // C].reshape(tile, Z) for k in range(2)], axis=-1
                )
                part = dot(wbd_ref[...], hidden).reshape(tile // C, C, 2 * Z) * gain[None] + bias
                for k in range(2):
                    pre_ref[x + k, y:y + tile // C] = part[:, :, k * Z:(k + 1) * Z]
            return carry
        lax.fori_loop(low, high, go, 0)

    pairs = xl // 2
    early, mid = pairs // 8, pairs // 2
    skip_cells(0, early)
    send_half(halves - 1)

    ti_ref[...] = spread_table(txi_ref[...], 2 * xl * MZ, lambda j: div(j, MZ))
    DS = 8 if per_dl(dl, n_col, halves) else CH
    th_ref[...] = spread_table(
        tyi_ref[...], 2 * MY * DS,
        (lambda j: div(j, DS)) if DS < CH else
        (lambda j: div(j, per * kyl * dl) * kyl + mod(div(j, dl), kyl)),
    )

    def put_gx(first, value):
        for n in range(gx_ref.shape[0]):
            gx_ref[n, pl.ds(first, MZ), :] = value[:, n * gx_ref.shape[2]:(n + 1) * gx_ref.shape[2]]

    wide = 2 * xl * MZ
    band(put_gx, ti_ref, 4 * MX, MZ, iota((MZ, wide), 0) == mod(iota((MZ, wide), 1), MZ))

    def put_hy(first, value):
        hy_ref[pl.ds(first, DS), :] = value

    j = iota((DS, 2 * MY * DS), 1)
    chan = mod(j, DS) if DS < CH else mod(div(j, kyl * dl), per) * dl + mod(j, dl)
    band(put_hy, th_ref, yl, DS, iota((DS, 2 * MY * DS), 0) == chan)
    skip_cells(early, early + mid)

    sums = {}
    for h in range(halves):
        total = send_ref[h, gx, hi].astype(F32)
        for i in range(1, peers):
            scatter(h, i).wait_recv()
            total = total + recv_ref[h, i].astype(F32)
        spec = total.astype(BF).astype(F32)
        re, im = spec[:, :L // 2], spec[:, L // 2:]
        re = jnp.concatenate([re, re], axis=-1)
        im = jnp.concatenate([im, im], axis=-1)
        for a in range(n_col):
            for k in range(kyl):
                if h == 0 and a > 0:
                    share(n_col - a, k).wait_recv()
                rows, chans = slice(k * CH, (k + 1) * CH), slice(h * CH, (h + 1) * CH)
                weight = wa_ref[side(a), k, :, chans].astype(F32)
                new = [jnp.sum(v[rows][None] * weight, axis=1) for v in (re, im)]
                old = sums.get((a, k))
                sums[a, k] = new if old is None else [x + y for x, y in zip(old, new)]
    for k in range(kyl):
        mixed = []
        for a in range(n_col):
            first, second = sums[a, k]
            turned_second = jnp.concatenate(
                [-second[:, L // 2:], second[:, :L // 2]], axis=-1
            )
            mixed.append(first + turned_second)
        centre = sum(jnp.sum(m, axis=0, keepdims=True) for m in mixed) * (1.0 / C)
        for a in range(n_col):
            mix_ref[side(a), k] = ((mixed[a] - centre) * gcol_ref[side(a)]).astype(BF)

    def send_modes(h):
        loop(1, peers, lambda i: gather(h, i).start())
        relay(h, 0).start()

    def sent_modes(h):
        loop(1, peers, lambda i: gather(h, i).wait_send())
        relay(h, 0).wait_send()

    send_modes(0)
    modes_ref[gx, gy] = mix_ref[...]
    skip_cells(early + mid, pairs)
    for h in range(1, halves):
        sent_modes(h - 1)
        send_modes(h)
    for h in range(halves):
        swap(h).wait_send()
        loop(1, peers, lambda i: scatter(h, i).wait_send())
    for i in range(1, n_col):
        for k in range(kyl):
            share(i, k).wait_send()

    lanes = rows_ref.shape[-1]
    for h in range(halves):
        def pass_on(i):
            gather(h, i).wait_recv()
            relay(h, i).start()

        loop(1, peers, pass_on)
        relay(h, 0).wait_recv()
        loop(1, peers, lambda i: relay(h, i).wait_recv())
        part = jnp.concatenate(
            [
                jnp.concatenate([modes_ref[b, g, h * each:(h + 1) * each].reshape(span, L) for g in range(n_gy)], axis=0)
                for b in range(n_gx)
            ],
            axis=-1,
        )
        half = 2 * MX * MZ
        wide = 2 * xl * MZ
        part = jnp.concatenate(
            [dot(part, joined(gx_ref, cs * half, (cs + 1) * half)) for cs in range(2)], axis=0
        ).reshape(2 * MY, CH // DS, DS, wide)
        value = jnp.concatenate(
            [
                dot(hy_ref[...], part[:, e].reshape(2 * MY * DS, wide).astype(BF)).reshape(yl, DS, wide)
                for e in range(CH // DS)
            ],
            axis=1,
        ).astype(BF)
        for g in range(rows_ref.shape[0]):
            rows_ref[g, :, h * CH:(h + 1) * CH] = value[:, :, g * lanes:(g + 1) * lanes]
    sent_modes(halves - 1)
    for h in range(halves):
        loop(1, peers, lambda i: relay(h, i).wait_send())


def back_kernel(
    sizes, rows_ref, pre_ref, depth_ref, gain_ref, shift_ref, out_hbm,
    out_ref, part_ref, square_ref, sem,
):
    trips, G, yl, C, Z, cells, unroll = sizes
    tall, wide = cells * C, G * Z

    root = 0.5 ** 0.5
    diagonal = iota((C, C), 0) == iota((C, C), 1)
    shift = jnp.sum(jnp.where(diagonal, shift_ref[...], 0.0), 1, keepdims=True) * root
    shift = jnp.broadcast_to(shift, (C, Z)).reshape(1, C // 8, 8, Z)
    inverse = 1.0 / (jnp.sum(jnp.where(diagonal, gain_ref[...], 0.0), 1, keepdims=True) * root)
    inverse = jnp.broadcast_to(inverse, (C, Z)).reshape(1, C // 8, 8, Z)

    tiles = [(a, y) for a in range(unroll) for y in range(0, yl, cells)]

    def leave(i, slot, t):
        a, y = tiles[t]
        return pltpu.make_async_copy(
            out_ref.at[slot, pl.ds(a * G, G), pl.ds(y, cells)],
            out_hbm.at[pl.ds((i * unroll + a) * G, G), pl.ds(y, cells)], sem.at[slot, t],
        )

    def go(i, carry):
        slot = mod(i, 2)

        @pl.when(i >= 2)
        def _():
            for t in range(len(tiles)):
                leave(i - 2, slot, t).wait()

        def first(t):
            a, y = tiles[t]
            g = i * unroll + a
            part = dot(rows_ref[g, y:y + cells].reshape(tall, rows_ref.shape[-1]), depth_ref[...])
            for k in range(G):
                at = slice(k * Z, (k + 1) * Z)
                value = part[:, at] + pre_ref[g * G + k, y:y + cells].reshape(tall, Z)
                part_ref[t % 2, k] = value
                value = value.reshape(cells, C // 8, 8, Z) * inverse
                value = jnp.sum(value * value, axis=1)
                square_ref[t % 2, k] = value.reshape(8 * cells, Z).astype(F32)

        def second(t):
            a, y = tiles[t]
            square = jnp.concatenate([square_ref[t % 2, k] for k in range(G)], axis=-1)
            spread = jnp.sum(square.reshape(cells, 8, wide), axis=1, keepdims=True) * (1.0 / C)
            spread = lax.rsqrt(spread + norm_eps)
            spread = jnp.broadcast_to(spread, (cells, 8, wide)).reshape(cells, 1, 8, wide)
            for k in range(G):
                at = slice(k * Z, (k + 1) * Z)
                value = part_ref[t % 2, k].reshape(cells, C // 8, 8, Z)
                value = (value * spread[..., at] + shift).reshape(cells, C, Z).astype(BF)
                value = (value * root).astype(BF) * (1.0 + lax.erf(value)).astype(BF)
                out_ref[slot, a * G + k, y:y + cells] = value

        for t in range(len(tiles) + 1):
            if t < len(tiles):
                first(t)
            if t >= 1:
                second(t - 1)
                leave(i, slot, t - 1).start()
        return carry

    lax.fori_loop(0, trips, go, 0)
    for i in range(max(0, trips - 2), trips):
        for t in range(len(tiles)):
            leave(i, i % 2, t).wait()


def build(mesh):
    n_gx, n_gy, n_col = (mesh.shape[a] for a in ("gx", "gy", "col"))

    def local(fields, spectral, skip_weight, skip_bias, norm_gain, norm_shift):
        hidden = fields[0]
        xl, yl, C, Z = hidden.shape
        weights = spectral[0]
        kxl, kyl, _, _, dl, MZ = weights.shape
        X, Y, MX, MY = xl * n_gx, yl * n_gy, kxl * n_gx, kyl * n_gy
        G = min(8, xl)
        steps = xl // G
        L = 2 * kxl * MZ
        n_hi = n_gy // 2
        peers = n_gx * n_hi
        G2 = min(4, xl)

        cz, sz = cos_sin(np.arange(Z), np.arange(MZ), Z)
        forward = np.concatenate([cz, -sz], axis=1)
        depth_forward = np.kron(np.eye(G), forward)
        backward = np.concatenate([cz.T, -sz.T], axis=0) / math.sqrt(MX * MY * MZ)
        depth_backward = np.kron(np.eye(G2), backward)
        cy, sy = cos_sin(np.arange(Y), signed(MY), Y)
        tyf = np.stack([cy, sy]).reshape(2, n_gy, yl, MY).transpose(1, 0, 3, 2)
        tyf = tyf.reshape(n_gy, 2 * MY, yl)
        tyi = np.stack([cy, sy]).reshape(2, n_gy, yl, MY).transpose(1, 2, 0, 3)
        tyi = tyi.reshape(n_gy, yl, 2 * MY)
        cx, sx = cos_sin(np.arange(X), signed(MX), X)
        f = np.stack([
            np.stack([np.stack([cx, -sx], 1), np.stack([sx, cx], 1)], 1),
            np.stack([np.stack([-sx, -cx], 1), np.stack([cx, -sx], 1)], 1),
        ]) / math.sqrt(X * Y * Z)
        f = f.reshape(2, n_gx, xl, 2, 2, n_gx, kxl).transpose(1, 0, 2, 3, 5, 4, 6)
        txf = f.reshape(n_gx, 4 * xl, 2 * MX)
        b = np.stack([
            np.stack([np.stack([cx, sx]), np.stack([-sx, cx])]),
            np.stack([np.stack([-sx, cx]), np.stack([-cx, -sx])]),
        ])
        b = b.reshape(2, 2, 2, n_gx, xl, n_gx, kxl).transpose(3, 0, 5, 1, 6, 4, 2)
        txi = b.reshape(n_gx, 4 * MX, 2 * xl)
        const = lambda a: jnp.asarray(a.astype(np.float32)).astype(BF)

        halves = 2 if C % 32 == 0 and n_col % 2 == 0 else 1
        CH = C // halves
        CS = 8 if CH % 8 == 0 else CH
        DS = 8 if per_dl(dl, n_col, halves) else CH
        turned = jnp.transpose(weights, (0, 1, 2, 4, 5, 3))
        tile = min(256, yl * C)

        sizes = (n_gx, n_gy, n_col, xl, yl, C, MY, MZ, kxl, kyl, dl, G, steps, halves, tile)
        tables = [const(t) for t in (depth_forward, tyf, txf, txi, tyi)]
        inside = pl.BlockSpec(memory_space=pltpu.VMEM)
        outside = pl.BlockSpec(memory_space=pltpu.HBM)
        rows_both, pre = pl.pallas_call(
            functools.partial(front_kernel, sizes),
            out_shape=(
                pltpu.VMEM((xl // G2, yl, C, G2 * 2 * MZ), BF),
                pltpu.VMEM((xl, yl, C, Z), F32),
            ),
            in_specs=[outside] * (len(tables) + 5),
            out_specs=(inside, inside),
            scratch_shapes=[
                pltpu.VMEM((xl, yl, C, Z), BF),
                pltpu.VMEM((2 * MY * CS, yl * CS), BF),
                pltpu.VMEM(columns(4 * xl * MZ, 2 * MX * MZ), BF),
                pltpu.VMEM((2, CH // CS, yl * CS, G * 2 * MZ), BF),
                pltpu.VMEM((2, steps, 2 * MY * CH, G * 2 * MZ), BF),
                pltpu.VMEM((2, n_gx, MY * CH, L), F32),
                pltpu.VMEM((halves, n_hi, n_gx, kyl * CH, L), BF),
                pltpu.VMEM((halves, n_hi, n_gx, kyl * CH, L), BF),
                pltpu.VMEM((halves, n_gx, n_hi, kyl * CH, L), BF),
                pltpu.VMEM((halves, peers, kyl * CH, L), BF),
                pltpu.VMEM((n_col, kyl, dl, L), BF),
                pltpu.VMEM((n_gx, n_gy, n_col, kyl, dl, L), BF),
                pltpu.VMEM(columns(4 * MX * MZ, 2 * xl * MZ), BF),
                pltpu.VMEM((yl * DS, 2 * MY * DS), BF),
                pltpu.VMEM(turned.shape, BF),
                pltpu.VMEM((n_col, kyl, dl, C, L), BF),
                pltpu.VMEM((tile, tile), BF),
                pltpu.VMEM((2 * MY, yl * CS), F32),
                pltpu.VMEM((4 * xl, 2 * MX * MZ), F32),
                pltpu.VMEM((4 * MX, 2 * xl * MZ), F32),
                pltpu.VMEM((yl, 2 * MY * DS), F32),
                pltpu.SemaphoreType.DMA((halves, steps)),
                pltpu.SemaphoreType.DMA,
                pltpu.SemaphoreType.DMA((halves,)),
                pltpu.SemaphoreType.DMA((halves,)),
                pltpu.SemaphoreType.DMA((halves, peers)),
                pltpu.SemaphoreType.DMA((halves, peers)),
                pltpu.SemaphoreType.DMA((n_col, kyl)),
                pltpu.SemaphoreType.DMA((n_col, kyl)),
                pltpu.SemaphoreType.DMA((halves, peers)),
                pltpu.SemaphoreType.DMA((halves, peers)),
                pltpu.SemaphoreType.DMA((halves, peers)),
                pltpu.SemaphoreType.DMA((halves, peers)),
                pltpu.VMEM(tables[0].shape, BF),
                pltpu.VMEM(tables[1].shape[1:], BF),
                pltpu.VMEM(tables[2].shape[1:], BF),
                pltpu.VMEM(tables[3].shape[1:], BF),
                pltpu.VMEM(tables[4].shape[1:], BF),
                pltpu.VMEM((C, C), BF),
                pltpu.VMEM((1, C), F32),
                pltpu.VMEM((1, C), F32),
                pltpu.VMEM((n_col, dl, L), F32),
                pltpu.SemaphoreType.DMA((8,)),
            ],
            compiler_params=pltpu.CompilerParams(
                collective_id=0, has_side_effects=True, vmem_limit_bytes=40 * 2**20,
            ),
            name="front",
        )(hidden, turned, *tables, skip_weight[0], skip_bias, norm_gain)

        groups = xl // G2
        cells = min(8, yl)
        unroll = 1 if groups % 1 == 0 else 1
        out = pl.pallas_call(
            functools.partial(back_kernel, (groups // unroll, G2, yl, C, Z, cells, unroll)),
            out_shape=jax.ShapeDtypeStruct(hidden.shape, BF),
            in_specs=[inside] * 5,
            out_specs=outside,
            scratch_shapes=[
                pltpu.VMEM((2, unroll * G2, yl, C, Z), BF),
                pltpu.VMEM((2, G2, cells * C, Z), F32),
                pltpu.VMEM((2, G2, 8 * cells, Z), F32),
                pltpu.SemaphoreType.DMA((2, unroll * yl // cells)),
            ],
            compiler_params=pltpu.CompilerParams(vmem_limit_bytes=12 * 2**20),
            name="back",
        )(rows_both, pre, const(depth_backward), norm_gain, norm_shift)
        return out[None]

    return local


def solution(mesh):
    placed = (
        P("col", "gx", "gy", None, None),
        P(None, "gx", "gy", None, None, "col", None),
        P(), P(), P(), P(),
    )
    return jax.shard_map(
        build(mesh), mesh=mesh, in_specs=placed,
        out_specs=P("col", "gx", "gy", None, None), check_vma=False,
    )
```
